32 devices in a mesh: expert: 16 (over z, y, core), token: 2 (over x).
Axes of the slice: x: 2, y: 2, z: 4, core: 2. Of those that a mesh axis runs over, the one named last changes fastest.
Arguments:
- cotangent: bfloat16 [4096, 2048], P(('expert', 'token')), may hold values from -6 to 6
- expert_ids: int32 [4096, 6], P(('expert', 'token')), may hold values from 0 to 15, all different within a row; in each aligned block of 128 rows (0 to 127, 128 to 255, ...) at most 56 rows name the same one
- gate_values: float32 [4096, 6], P(('expert', 'token')), may hold values from 0.05 to 0.45
- hidden_pre: bfloat16 [16, 1792, 768], P('expert', 'token'), may hold values from -8 to 8
- up_weight: bfloat16 [16, 2048, 768], P('expert'), may hold values from -0.125 to 0.125
- down_weight: bfloat16 [16, 2048, 768], P('expert'), may hold values from -0.21875 to 0.21875
Outputs:
- input_grad: bfloat16 [4096, 2048], P(('expert', 'token'))
- down_grad: bfloat16 [16, 2048, 768], P('expert', 'token')
The draws below stay inside these ranges and needn't reach their ends.
Inputs may be any that keep to these rules, and one draw needn't show every extreme that they name: `expert_ids`: each row names 6 different experts. Among the 128 rows of one device no expert is named more than 56 times, and in every draw some expert is named exactly 56 times by the rows of some device.
All inputs are finite; a program needn't handle non-finite values.
Results may differ from the reference program's by a relative error of at most 0.007.
Values may be sent and summed in bfloat16 or wider, within the bound.
A program may use at most 128 MiB of HBM per device.

```python
import math
import jax
import jax.numpy as jnp
import numpy as np
from jax import lax

D = 2048
H = 768
TOP = 6
T_DEV = 128
EXPERTS = 16
CAP = 56
SLOTS = 1792
TOKENS = 4096
N_TOKEN = 2


def steps_of(rng, extent, shards, smallest, largest):
    factor_of = 1.0
    for dim, shards_of in shards:
        steps = jax.random.uniform(jax.random.fold_in(jax.random.fold_in(rng, 6), dim), (shards_of,), jnp.float32, smallest / len(shards), largest / len(shards))
        factor_of = factor_of * jnp.repeat(jnp.exp(steps), extent[dim] // shards_of).reshape((-1,) + (1,) * (len(extent) - 1 - dim))
    return factor_of


def assign_block(rng, own, number, rows, number_of, top, reach, lean):
    ranking = jax.random.permutation(rng, number_of)
    crowded, common = shares(number_of, rows * top, reach, lean, True), shares(number_of, rows * top, reach, lean, False)
    places = jnp.arange(number_of)

    def named(tallies, offset_by):
        used = int((tallies > 0).sum())
        fixed = max(1, used // 4)
        passed = fixed + (places - fixed + offset_by * (used - fixed)) % max(1, number_of - fixed)
        return jnp.zeros((number_of,), jnp.int32).at[ranking[jnp.where(places < fixed, places, passed)]].set(jnp.asarray(tallies, jnp.int32))

    tallies = jnp.where(number % 4 == 0, named(crowded, number // 4), named(common, number - number // 4 - 1))
    mixed = jax.random.permutation(jax.random.fold_in(own, 3), number_of)
    donor, receiver = mixed[0:number_of // 2 * 2:2], mixed[1:number_of // 2 * 2:2]
    margin = jnp.minimum(tallies[donor] - 1, reach - tallies[receiver]) // 2
    margin = jnp.where((donor == ranking[0]) | (receiver == ranking[0]) | (tallies[receiver] == 0), 0, jnp.maximum(margin, 0))
    passed = jax.random.randint(jax.random.fold_in(own, 4), (number_of // 2,), 0, 1 << 20) % (margin + 1)
    tallies = tallies.at[donor].add(-passed).at[receiver].add(passed)
    members = jnp.searchsorted(jnp.cumsum(tallies), jnp.arange(rows * top), side="right").astype(jnp.int32)
    listing = members.reshape(top, rows).T
    listing = listing[jax.random.permutation(jax.random.fold_in(own, 1), rows)]
    offset_by = jax.random.randint(jax.random.fold_in(own, 2), (rows, 1), 0, top)
    return jnp.take_along_axis(listing, (jnp.arange(top)[None, :] + offset_by) % top, axis=1)


def shares(amount, total, bound, lean, full):
    loads = [(1 << 20) // math.isqrt(grade ** lean) + 1 for grade in range(1, amount + 1)]
    largest = bound if full else min(bound, max(-(-total // amount), total * loads[0] // sum(loads)))
    least = 1 if total - largest >= amount - 1 else 0
    holding, rest = [largest] + [least] * (amount - 1), total - largest - least * (amount - 1)
    while rest > 0:
        free = [i for i in range(1, amount) if holding[i] < largest] or [i for i in range(1, amount) if holding[i] < bound]
        pool, budget = sum([loads[i] for i in free]), rest
        for i in free:
            addition = min(bound - holding[i], max(1, budget * loads[i] // pool), rest)
            holding[i] = holding[i] + addition
            rest = rest - addition
    return np.array(holding)


def scatter_about(rng, dims, scale, bound, split=(), kind=jnp.bfloat16):
    factor_of = steps_of(rng, dims, split, -0.22, 0.18) if split else 1.0
    values = jax.random.normal(rng, dims, jnp.float32) * scale * factor_of
    return jnp.minimum(jnp.maximum(values, -bound), bound).astype(kind)


def setup_inputs(seed: int = 0) -> dict:
    splits = jax.random.split(jax.random.key(seed), 7)
    cotangent = scatter_about(splits[0], (TOKENS, D), 1.0, 6.0, ((0, 32),))
    expert_ids_keys = jax.random.split(jax.random.fold_in(splits[1], 1), TOKENS // T_DEV)
    expert_ids_turns = jax.random.permutation(jax.random.fold_in(splits[1], 3), TOKENS // T_DEV)
    expert_ids = jax.vmap(lambda own, number: assign_block(jax.random.fold_in(splits[1], 2), own, number, T_DEV, EXPERTS, TOP, CAP, 2))(expert_ids_keys, expert_ids_turns).reshape((TOKENS, TOP))
    gate_values = jnp.clip(0.05 + 0.39999999 * jax.random.uniform(splits[2], (TOKENS, TOP), jnp.float32) ** steps_of(splits[2], (TOKENS, TOP), ((0, 32),), -0.2, 0.2), 0.05, 0.45)
    hidden_pre = scatter_about(splits[3], (EXPERTS, SLOTS, H), 1.5, 8.0, ((0, 16), (1, 2)))
    up_weight = scatter_about(splits[4], (EXPERTS, D, H), D ** -0.5, 0.125, ((0, 16),))
    down_weight = scatter_about(splits[5], (EXPERTS, D, H), H ** -0.5, 0.21875, ((0, 16),))
    return {"cotangent": cotangent, "expert_ids": expert_ids, "gate_values": gate_values, "hidden_pre": hidden_pre, "up_weight": up_weight, "down_weight": down_weight}


grad_scale = 0.03125
root_half = 0.7071067811865476
inv_root_two_pi = 0.3989422804014327


def slope_and_act(hidden_rows):
    values = hidden_rows.astype(jnp.float32)
    normal_cdf = 0.5 * (1.0 + lax.erf(values * root_half))
    density = inv_root_two_pi * jnp.exp(-0.5 * values * values)
    slopes = normal_cdf + values * density
    active = (values * normal_cdf).astype(jnp.bfloat16)
    return slopes, active


def slot_tables(expert_ids, gate_values, slot_count):
    top_count = expert_ids.shape[1]
    blocks = expert_ids.shape[0] // T_DEV
    grouped = expert_ids.reshape(blocks, T_DEV * top_count)
    one_hot = (grouped[:, :, None] == jnp.arange(EXPERTS, dtype=jnp.int32)[None, None, :]).astype(jnp.int32)
    earlier = jnp.cumsum(one_hot, axis=1) - one_hot
    rank_in = jnp.sum(earlier * one_hot, axis=2).astype(jnp.int32)
    block_ids = jnp.arange(blocks, dtype=jnp.int32)[:, None]
    slot_row = (block_ids % N_TOKEN) * (EXPERTS * CAP) + (block_ids // N_TOKEN) * CAP + rank_in
    token_ids = block_ids * T_DEV + jnp.arange(T_DEV * top_count, dtype=jnp.int32)[None, :] // top_count
    flat_expert = grouped.reshape(-1).astype(jnp.int32)
    flat_slot = slot_row.reshape(-1).astype(jnp.int32)
    slot_token = jnp.zeros((EXPERTS, slot_count), jnp.int32).at[flat_expert, flat_slot].set(token_ids.reshape(-1).astype(jnp.int32))
    slot_gate = jnp.zeros((EXPERTS, slot_count), jnp.float32).at[flat_expert, flat_slot].set(gate_values.reshape(-1))
    slot_live = jnp.zeros((EXPERTS, slot_count), jnp.float32).at[flat_expert, flat_slot].set(jnp.ones_like(gate_values.reshape(-1)))
    return slot_token, slot_gate, slot_live


def apply_transpose(token_rows, slot_token, slot_gate, slot_live, hidden_pre, up_weight, down_weight):
    def per_expert(summed, stacked):
        token_ids, gate_e, live_e, hidden_e, up_e, down_e = stacked
        slopes, unused_act = slope_and_act(hidden_e)
        gathered = jnp.take(token_rows, token_ids, axis=0)
        gathered = jnp.where(live_e[:, None] > 0.5, gathered, jnp.zeros_like(gathered))
        inner_prod = jnp.dot(gathered, down_e, preferred_element_type=jnp.float32)
        scaled = (inner_prod * slopes).astype(jnp.bfloat16)
        pieces = jnp.dot(scaled, up_e.T, preferred_element_type=jnp.float32).astype(jnp.bfloat16)
        weighted = pieces.astype(jnp.float32) * gate_e[:, None]
        summed = summed.at[token_ids].add(weighted)
        return summed, jnp.zeros((), jnp.float32)

    initial = jnp.zeros(token_rows.shape, jnp.float32)
    summed, unused_out = lax.scan(per_expert, initial, (slot_token, slot_gate, slot_live, hidden_pre, up_weight, down_weight))
    return summed.astype(jnp.bfloat16)


def reference(cotangent, expert_ids, gate_values, hidden_pre, up_weight, down_weight):
    slot_token, slot_gate, slot_live = slot_tables(expert_ids, gate_values, hidden_pre.shape[1])
    first_term = apply_transpose(cotangent, slot_token, slot_gate, slot_live, hidden_pre, up_weight, down_weight)
    second = apply_transpose(first_term, slot_token, slot_gate, slot_live, hidden_pre, up_weight, down_weight)
    input_grad = (cotangent.astype(jnp.float32) + first_term.astype(jnp.float32) + second.astype(jnp.float32)).astype(jnp.bfloat16)

    def grad_expert(carried, stacked):
        token_ids, gate_e, hidden_e = stacked
        unused_slope, active = slope_and_act(hidden_e)
        picked = jnp.take(input_grad, token_ids, axis=0).astype(jnp.float32)
        routed = (picked * gate_e[:, None]).astype(jnp.bfloat16)
        grad_e = jnp.dot(routed.T, active, preferred_element_type=jnp.float32)
        return carried, (grad_e * grad_scale).astype(jnp.bfloat16)

    unused_carry, down_grad = lax.scan(grad_expert, jnp.zeros((), jnp.float32), (slot_token, slot_gate, hidden_pre))
    return input_grad, down_grad
```

```python
import functools

import jax
import jax.numpy as jnp
from jax import lax
from jax.experimental import pallas as pl
from jax.experimental.pallas import tpu as pltpu
from jax.sharding import PartitionSpec as P

grad_scale = 0.03125
root_half = 0.7071067811865476
inv_root_two_pi = 0.3989422804014327


def slope_and_act(hidden_rows):
    values = hidden_rows.astype(jnp.float32)
    normal_cdf = 0.5 * (1.0 + lax.erf(values * root_half))
    density = inv_root_two_pi * jnp.exp(-0.5 * values * values)
    slopes = normal_cdf + values * density
    active = (values * normal_cdf).astype(jnp.bfloat16)
    return (slopes, active)


def slot_tables(ids, gates, capacity):
    me = lax.axis_index("expert")
    hit = ids == me
    match = jnp.any(hit, axis=2)
    gate = jnp.sum(jnp.where(hit, gates, 0.0), axis=2)
    rows = ids.shape[1]
    order = jnp.arange(rows, dtype=jnp.int32)
    before = (order[:, None] < order[None, :]).astype(jnp.bfloat16)
    rank = jnp.dot(match.astype(jnp.bfloat16), before, preferred_element_type=jnp.float32)
    rank = jnp.where(match, rank.astype(jnp.int32), -1)
    chosen = rank[:, None, :] == jnp.arange(capacity, dtype=jnp.int32)[None, :, None]
    slot_gate = jnp.sum(jnp.where(chosen, gate[:, None, :], 0.0), axis=2)
    return chosen.astype(jnp.bfloat16), slot_gate


MESH = pl.DeviceIdType.MESH


def ring_place(experts):
    chips = experts // 2
    side = chips // 2
    me = lax.axis_index("expert")
    core = me % 2
    chip = me // 2
    row, odd = chip // 2, chip % 2
    place = row + odd * (chips - 1 - 2 * row)

    def device(at):
        at = (at + 2 * chips) % chips
        back = at // side
        return ((at + back * (chips - 1 - 2 * at)) * 2 + back) * 2

    return place, core, device


def ring_messages(chips):
    side = chips // 2
    return [
        [(d, h) for d in range(1, side + 1) for h in range(2) if d < side or h == way]
        for way in range(2)
    ]


def greet(peers):
    barrier = pltpu.get_barrier_semaphore()
    for peer in peers:
        pl.semaphore_signal(barrier, inc=1, device_id={"expert": peer}, device_id_type=MESH)
    pl.semaphore_wait(barrier, len(peers))


def send(src, dst, send_sem, recv_sem, peer):
    return pltpu.make_async_remote_copy(
        src_ref=src,
        dst_ref=dst,
        send_sem=send_sem,
        recv_sem=recv_sem,
        device_id={"expert": peer},
        device_id_type=MESH,
    )


def gather_kernel(experts, count, *refs):
    mine, outs = refs[:count], refs[count : 2 * count]
    hop_send, hop_recv, sib_send, sib_recv, own_sem, cross_sems = refs[2 * count :]
    chips = experts // 2
    messages = ring_messages(chips)
    place, core, device = ring_place(experts)
    me = lax.axis_index("expert")
    sibling = me + 1 - 2 * core
    peers = (device(place + 1) + core, device(place - 1) + core)
    own = [pltpu.make_async_copy(mine[i], outs[i].at[me], own_sem.at[i]) for i in range(count)]
    for copy in own:
        copy.start()
    greet(peers + (sibling,))

    def rows_of(i, half):
        size = mine[i].shape[0] // 2
        return pl.ds(half * size, size)

    def hop(i, way, index):
        distance, half = messages[way][index]
        sign = 1 - 2 * way
        rows = rows_of(i, half)
        origin = device(place - sign * (distance - 1)) + core
        src = mine[i].at[rows] if distance == 1 else outs[i].at[origin, rows]
        return send(
            src,
            outs[i].at[origin, rows],
            hop_send.at[i, way, index],
            hop_recv.at[i, way, index],
            peers[way],
        )

    def landed(i, way, index, which):
        distance, half = messages[way][index]
        origin = device(place - (1 - 2 * way) * distance) + which
        return outs[i].at[origin, rows_of(i, half)]

    def across(i, way, index, which):
        block = landed(i, way, index, which)
        return send(
            block, block, sib_send.at[i, way, index], sib_recv.at[i, way, index], sibling
        )

    for index in range(2):
        for way in range(2):
            for i in range(count):
                if index < len(messages[way]) and messages[way][index][0] == 1:
                    hop(i, way, index).start()
    cross = [
        send(mine[i], outs[i].at[me], cross_sems.at[0, i], cross_sems.at[1, i], sibling)
        for i in range(count)
    ]
    for copy in cross:
        copy.start()
    for index in range(len(messages[0])):
        for way in range(2):
            distance, half = messages[way][index]
            for i in range(count):
                block = landed(i, way, index, core)
                send(
                    block,
                    block,
                    hop_send.at[i, way, index],
                    hop_recv.at[i, way, index],
                    peers[way],
                ).wait_recv()
                if (distance + 1, half) in messages[way]:
                    hop(i, way, messages[way].index((distance + 1, half))).start()
                across(i, way, index, core).start()
    for i in range(count):
        own[i].wait()
        cross[i].wait_send()
        send(
            mine[i], outs[i].at[sibling], cross_sems.at[0, i], cross_sems.at[1, i], sibling
        ).wait_recv()
        for way in range(2):
            for index in range(len(messages[way])):
                hop(i, way, index).wait_send()
                across(i, way, index, core).wait_send()
                across(i, way, index, 1 - core).wait_recv()


def gather_rows(arrays, name):
    experts = lax.axis_size("expert")
    count = len(arrays)
    steps = len(ring_messages(experts // 2)[0])
    dma = pltpu.SemaphoreType.DMA
    return pl.pallas_call(
        functools.partial(gather_kernel, experts, count),
        out_shape=[jax.ShapeDtypeStruct((experts,) + a.shape, a.dtype) for a in arrays],
        in_specs=[pl.BlockSpec(memory_space=pltpu.VMEM)] * count,
        out_specs=[pl.BlockSpec(memory_space=pl.ANY)] * count,
        scratch_shapes=[
            dma((count, 2, steps)),
            dma((count, 2, steps)),
            dma((count, 2, steps)),
            dma((count, 2, steps)),
            dma((count,)),
            dma((2, count)),
        ],
        compiler_params=pltpu.CompilerParams(
            collective_id=name, has_side_effects=True, vmem_limit_bytes=8 * 1024 * 1024
        ),
        cost_estimate=pl.CostEstimate(
            flops=20_000_000_000, bytes_accessed=20_000_000, transcendentals=0
        ),
        name="gather" + str(name),
    )(*arrays)


def scatter_kernel(
    experts, parts, out, own, other, came, own_sem, sib_send, sib_recv, hop_send, hop_recv
):
    chips = experts // 2
    side = chips // 2
    messages = ring_messages(chips)
    place, core, device = ring_place(experts)
    me = lax.axis_index("expert")
    sibling = me + 1 - 2 * core
    peers = (device(place + 1) + core, device(place - 1) + core)
    size = out.shape[0] // 2
    order = [side]
    for d in range(side - 1, 0, -1):
        order += [d, chips - d]
    order += [0]
    loads = {
        k: pltpu.make_async_copy(parts.at[device(place + k) + core], own.at[k], own_sem.at[k])
        for k in order
    }
    for k in order:
        loads[k].start()
    greet(peers + (sibling,))
    gifts = {
        k: send(
            parts.at[device(place + k) + 1 - core],
            other.at[k],
            sib_send.at[k],
            sib_recv.at[k],
            sibling,
        )
        for k in order
    }
    for k in order:
        gifts[k].start()

    def hop(way, message):
        distance, half = message
        k = distance if way == 0 else chips - distance
        rows = pl.ds(half * size, size)
        index = messages[way].index(message)
        return send(
            own.at[k, rows],
            came.at[way, distance - 1, rows],
            hop_send.at[way, index],
            hop_recv.at[way, index],
            peers[way],
        )

    step = 16

    def add_up(k, half, more, target):
        @pl.loop(0, size // step)
        def _(at):
            rows = pl.ds(pl.multiple_of(half * size + at * step, step), step)
            total = own[k, rows, :].astype(jnp.float32) + other[k, rows, :].astype(jnp.float32)
            for way, slot in more:
                total = total + came[way, slot, rows, :].astype(jnp.float32)
            if target is None:
                own[k, rows, :] = total.astype(own.dtype)
            else:
                target[rows, :] = total.astype(target.dtype)

    ready = set()

    def get(k):
        if k not in ready:
            ready.add(k)
            loads[k].wait()
            gifts[k].wait_recv()

    for distance in range(side, 0, -1):
        for half in range(2):
            for way in range(2):
                if (distance, half) not in messages[way]:
                    continue
                k = distance if way == 0 else chips - distance
                get(k)
                more = []
                if (distance + 1, half) in messages[way]:
                    hop(way, (distance + 1, half)).wait_recv()
                    more = [(way, distance)]
                add_up(k, half, more, None)
                hop(way, (distance, half)).start()
    get(0)
    for half in range(2):
        more = []
        for way in range(2):
            if (1, half) in messages[way]:
                hop(way, (1, half)).wait_recv()
                more.append((way, 0))
        add_up(0, half, more, out)
    for k in order:
        gifts[k].wait_send()
    for way in range(2):
        for message in messages[way]:
            hop(way, message).wait_send()


def scatter_sum(blocks):
    experts, rows, width = blocks.shape
    chips = experts // 2
    steps = len(ring_messages(chips)[0])
    dma = pltpu.SemaphoreType.DMA
    buffers = (3 * chips + 4) * rows * width * 2
    return pl.pallas_call(
        functools.partial(scatter_kernel, experts),
        out_shape=jax.ShapeDtypeStruct((rows, width), blocks.dtype),
        in_specs=[pl.BlockSpec(memory_space=pl.ANY)],
        out_specs=pl.BlockSpec(memory_space=pltpu.VMEM),
        scratch_shapes=[
            pltpu.VMEM((chips, rows, width), blocks.dtype),
            pltpu.VMEM((chips, rows, width), blocks.dtype),
            pltpu.VMEM((2, chips // 2, rows, width), blocks.dtype),
            dma((chips,)),
            dma((chips,)),
            dma((chips,)),
            dma((2, steps)),
            dma((2, steps)),
        ],
        compiler_params=pltpu.CompilerParams(
            collective_id=7, has_side_effects=True, vmem_limit_bytes=buffers + 2 * 1024 * 1024
        ),
        cost_estimate=pl.CostEstimate(
            flops=20_000_000_000, bytes_accessed=20_000_000, transcendentals=0
        ),
        name="scatter_sum",
    )(blocks)


def from_groups(make):
    groups = lax.axis_size("token")
    mine = lax.axis_index("token")
    taken = [make(mine)]
    for shift in range(1, groups):
        pairs = [(t, (t + shift) % groups) for t in range(groups)]
        taken.append(lax.ppermute(make((mine + shift) % groups), "token", pairs))
    return jnp.stack(taken)


def pick(sel, rows):
    return lax.dot_general(
        sel, rows, (((2,), (1,)), ((0,), (0,))), preferred_element_type=jnp.float32
    ).astype(jnp.bfloat16)


def transpose_jacobian(everyone, sel, slot_gate, slopes, up_weight, down_weight):
    blocks, capacity, rows = sel.shape
    picked = pick(sel, everyone).reshape(blocks * capacity, -1)
    inner_prod = jnp.dot(picked, down_weight, preferred_element_type=jnp.float32)
    scaled = (inner_prod * slopes).astype(jnp.bfloat16)
    pieces = lax.dot_general(
        scaled, up_weight, (((1,), (1,)), ((), ())), preferred_element_type=jnp.float32
    ).astype(jnp.bfloat16)
    weighted = (pieces.astype(jnp.float32) * slot_gate.reshape(-1, 1)).astype(jnp.bfloat16)
    spread = lax.dot_general(
        sel,
        weighted.reshape(blocks, capacity, -1),
        (((1,), (1,)), ((0,), (0,))),
        preferred_element_type=jnp.float32,
    ).astype(jnp.bfloat16)
    return scatter_sum(spread)


def staged(cotangent, expert_ids, gate_values, hidden_pre, up_weight, down_weight):
    experts = lax.axis_size("expert")
    groups = lax.axis_size("token")
    rows, width = cotangent.shape
    top = expert_ids.shape[1]
    padded = -(-2 * top // 16) * 16
    routes = jnp.concatenate([expert_ids.T.astype(jnp.float32), gate_values.T], axis=0)
    routes = jnp.pad(routes, ((0, padded - 2 * top), (0, 0)))
    routes = from_groups(lambda group: routes).reshape(groups * padded, rows)
    everyone, all_routes = gather_rows([cotangent, routes], 1)
    slopes, active = slope_and_act(hidden_pre[0])
    capacity = slopes.shape[0] // experts
    acts = from_groups(lambda group: active)
    all_routes = all_routes.reshape(experts * groups, padded, rows).transpose(0, 2, 1)
    all_sel, all_gate = slot_tables(
        all_routes[:, :, :top].astype(jnp.int32), all_routes[:, :, top : 2 * top], capacity
    )
    by_group = all_sel.reshape(experts, groups, capacity, rows)
    sel = by_group[:, 0]
    slot_gate = all_gate.reshape(experts, groups, capacity)[:, 0]
    first_term = transpose_jacobian(
        everyone, sel, slot_gate, slopes, up_weight[0], down_weight[0]
    )
    (everyone,) = gather_rows([first_term], 2)
    second = transpose_jacobian(everyone, sel, slot_gate, slopes, up_weight[0], down_weight[0])
    input_grad = (
        cotangent.astype(jnp.float32) + first_term.astype(jnp.float32) + second.astype(jnp.float32)
    ).astype(jnp.bfloat16)
    share = width // groups
    columns = from_groups(
        lambda group: lax.dynamic_slice_in_dim(input_grad, group * share, share, 1)
    ).reshape(groups * rows, share)
    (everyone,) = gather_rows([columns], 3)
    everyone = everyone.reshape(experts * groups, rows, share)
    picked = pick(all_sel, everyone)
    routed = (picked.astype(jnp.float32) * all_gate[:, :, None]).astype(jnp.bfloat16)
    acts = acts.reshape(groups, experts, capacity, -1).transpose(1, 0, 2, 3)
    summed = lax.dot_general(
        routed.reshape(experts * groups * capacity, -1),
        acts.reshape(experts * groups * capacity, -1),
        (((0,), (0,)), ((), ())),
        preferred_element_type=jnp.float32,
    )
    grad_out = (summed * grad_scale).astype(jnp.bfloat16)[None]
    return (input_grad, grad_out)


class Plan:
    def __init__(self, experts, groups, rows, width, hidden, slots):
        self.experts, self.groups, self.rows, self.width = experts, groups, rows, width
        self.hidden, self.slots = hidden, slots
        self.capacity = slots // experts
        self.planes = experts // 4
        self.chains = 2
        self.n = rows // self.chains
        self.split = width * 5 // 8 // 128 * 128

    def fits(self):
        lanes = 128
        whole = (
            self.groups == 2
            and self.experts % 4 == 0
            and 2 * self.experts <= lanes
            and self.planes <= 4
            and self.rows == lanes
            and self.n % 16 == 0
            and self.width % (4 * lanes) == 0
            and self.hidden % (2 * lanes) == 0
            and (2 * self.capacity) % 16 == 0
            and 2 * self.capacity <= 2 * lanes
            and self.slots <= self.rows * self.experts // self.chains
            and self.hidden <= self.width
        )
        return whole and self.bytes() <= 63 * 1024 * 1024

    def bytes(self):
        e, r, d, h, z = self.experts, self.rows, self.width, self.hidden, self.planes
        tokens = 2 * e * r * d * 2 + e * r * d * 2 + e * r * d
        lines = self.chains * (2 * z * self.n * (2 * d - self.split) + z * self.n * self.split) * 2
        return tokens + lines + 2 * d * h * 2 + e * r * h * (4 + 2 + 2) + 3 * r * d * 2 + d * h * 2 + d * h

    def semaphores(self):
        return self.chains * 34 * self.planes + 16 * self.planes


def fused_kernel(
    plan,
    cot,
    ids,
    gates,
    hidden_hbm,
    up_hbm,
    down_hbm,
    grad_in,
    grad_w,
    view,
    part,
    gift,
    came,
    came2,
    rung,
    last,
    slope,
    act,
    other,
    first,
    third,
    tabs,
    own_tab,
    turn,
    scaled,
    up,
    down,
    total,
    send_sems,
    recv_sems,
    load_sems,
):
    experts, planes, chains, n = plan.experts, plan.planes, plan.chains, plan.n
    width, hidden, cap, split = plan.width, plan.hidden, plan.capacity, plan.split
    top = ids.shape[1]
    half = width // 2
    rest = width - split
    me = lax.axis_index("expert")
    token = lax.axis_index("token")
    core = me % 2
    y = (me // 2) % 2
    z = me // 4
    has = {0: z > 0, 1: z < planes - 1}
    up_peer = {"expert": me + 4}
    down_peer = {"expert": me - 4}
    rung_peer = {"expert": me + 2 - 4 * y}
    sib_peer = {"expert": me + 1 - 2 * core}
    far_peer = {"token": 1 - token}
    sources = ((0, up_peer), (1, down_peer))
    c1, c2, full = pl.ds(0, split), pl.ds(split, rest), pl.ds(0, width)

    keys = {}

    def number(key):
        if key not in keys:
            keys[key] = len(keys)
            assert len(keys) <= plan.semaphores()
        return keys[key]

    def copy(key, src, dst, peer):
        at = number(key)
        return pltpu.make_async_remote_copy(
            src_ref=src,
            dst_ref=dst,
            send_sem=send_sems.at[at],
            recv_sem=recv_sems.at[at],
            device_id=peer,
            device_id_type=MESH,
        )

    def when(cond, action):
        if cond is None:
            action()
        else:
            pl.when(cond)(action)

    pending = {}

    def post(group, cond, key, src, dst, peer):
        when(cond, lambda: copy(key, src, dst, peer).start())
        pending.setdefault(group, []).append((cond, key, src, peer))

    def drain(group):
        for cond, key, src, peer in pending.pop(group, []):
            when(cond, lambda: copy(key, src, src, peer).wait_send())

    def arrive(cond, key, dst):
        when(cond, lambda: copy(key, dst, dst, sib_peer).wait_recv())

    def both(a, b):
        return b if a is None else (a if b is None else jnp.logical_and(a, b))

    def slot_of(p, yy, cc):
        return 4 * p + 2 * cc + yy

    def origin(way, d):
        return z - d if way == 0 else z + d

    def there(way, d):
        return z >= d if way == 0 else z + d < planes

    mine = slot_of(z, y, core)
    beside = slot_of(z, 1 - y, core)

    def gather(tag, at, src, whole):
        group = ("ag", tag)

        def start():
            drain(group)
            post(group, None, (tag, "rung"), src, at(mine, full), rung_peer)
            for way, peer in sources:
                post(group, has[1 - way], (tag, "rail", way, 1), src, at(mine, full), peer)
            post(group, None, (tag, "sib"), src, at(mine, full), sib_peer)

        def step(d):
            if d == 0:
                block = at(beside, full)
                arrive(None, (tag, "rung"), block)
                if not whole:
                    cut = at(beside, c2)
                    for way, peer in sources:
                        post(group, has[1 - way], (tag, "rail2", way, 1), cut, cut, peer)
                post(group, None, (tag, "sibp"), block, block, sib_peer)
                return
            for way, peer in sources:
                cond = there(way, d)
                o = slot_of(origin(way, d), y, core)
                block = at(o, full)
                arrive(cond, (tag, "rail", way, d), block)
                if d + 1 < planes:
                    on = both(cond, has[1 - way])
                    post(group, on, (tag, "rail", way, d + 1), block, block, peer)
                over = block if whole else at(o, c1)
                post(group, cond, (tag, "over", way, d), over, over, rung_peer)
                post(group, cond, (tag, "sib", way, d), block, block, sib_peer)
            if whole:
                return
            for way, peer in sources:
                cond = there(way, d)
                cut = at(slot_of(origin(way, d), 1 - y, core), c2)
                arrive(cond, (tag, "rail2", way, d), cut)
                if d + 1 < planes:
                    on = both(cond, has[1 - way])
                    post(group, on, (tag, "rail2", way, d + 1), cut, cut, peer)
                post(group, cond, (tag, "sib2", way, d), cut, cut, sib_peer)

        def across(d):
            for way in range(2):
                cond = there(way, d)
                cut = at(slot_of(origin(way, d), 1 - y, core), full if whole else c1)
                arrive(cond, (tag, "over", way, d), cut)
                post(group, cond, (tag, "sib1", way, d), cut, cut, sib_peer)

        def ready(d):
            if d == 0:
                arrive(None, (tag, "sib"), at(slot_of(z, y, 1 - core), full))
                arrive(None, (tag, "sibp"), at(slot_of(z, 1 - y, 1 - core), full))
                return
            for way in range(2):
                cond = there(way, d)
                p = origin(way, d)
                arrive(cond, (tag, "sib", way, d), at(slot_of(p, y, 1 - core), full))
                o = slot_of(p, 1 - y, 1 - core)
                if not whole:
                    arrive(cond, (tag, "sib2", way, d), at(o, c2))
                arrive(cond, (tag, "sib1", way, d), at(o, full if whole else c1))

        return start, step, across, ready

    def plane_at(i):
        low = jnp.minimum(z, planes - 1 - z)
        near = jnp.where(z < planes // 2, 1, -1)
        d = jnp.where(i <= 2 * low, (i + 1) // 2, i - low)
        sign = jnp.where(i <= 2 * low, near * (1 if i % 2 else -1), near)
        return z + sign * d if i else z

    tab_at = lambda slot, cols: tabs.at[slot]
    tab_start, tab_step, tab_across, tab_ready = gather("tab", tab_at, own_tab, True)

    sources_of = {0: cot, 1: first, 2: third}

    def chain_rows(chain):
        return pl.ds(chain * n, n)

    stages = {}
    for chain in range(chains):
        for f in range(3):

            def at(slot, cols, f=f, chain=chain):
                rows = pl.ds(pl.multiple_of(slot * n, n), n)
                return view.at[f % 2, chain, rows, cols]

            src = sources_of[f].at[chain_rows(chain)]
            stages[f, chain] = gather(chain, at, src, False)

    def start(f, chain):
        stages[f, chain][0]()
        rows = pl.ds(pl.multiple_of(mine * n, n), n)
        view[f % 2, chain, rows, :] = sources_of[f][chain_rows(chain), :]

    def hop(f, chain, d):
        stages[f, chain][1](d)

    def over(f, chain, d):
        if d:
            stages[f, chain][2](d)
        stages[f, chain][3](d)

    hidden_at = view.at[1, 0, pl.ds(0, plan.slots), pl.ds(0, hidden)]
    loads = [
        pltpu.make_async_copy(hidden_hbm, hidden_at, load_sems.at[0]),
        pltpu.make_async_copy(down_hbm, down, load_sems.at[1]),
        pltpu.make_async_copy(up_hbm, up, load_sems.at[2]),
    ]

    def make_table():
        lanes = plan.rows
        shape = (plan.rows, lanes)
        lane = lax.broadcasted_iota(jnp.int32, shape, 1)
        row = lax.broadcasted_iota(jnp.int32, shape, 0)
        match = jnp.zeros(shape, jnp.float32)
        gate = jnp.zeros(shape, jnp.float32)
        for k in range(top):
            name = ids[:, k : k + 1]
            match = match + jnp.where(name == lane, 1.0, 0.0)
            gate = gate + jnp.where(name + experts == lane, gates[:, k : k + 1], 0.0)
        before = jnp.where(lane < row, 1.0, 0.0).astype(jnp.bfloat16)
        rank = jnp.dot(before, match.astype(jnp.bfloat16), preferred_element_type=jnp.float32)
        rank = jnp.where(match > 0.5, rank, -4.0 * lanes)
        table = jnp.where(lane < experts, rank, gate).T
        own_tab[...] = table[: 2 * experts, :]
        tabs[mine] = table[: 2 * experts, :]

    tile = 256

    def prepare(i):
        p = plane_at(i)
        for j in range(4):
            turn[pl.ds(j, 1), :] = tabs[4 * p + j, pl.ds(me, 1), :]
            turn[pl.ds(4 + j, 1), :] = tabs[4 * p + j, pl.ds(experts + me, 1), :]
        turned = turn[...].T
        spot = lax.broadcasted_iota(jnp.int32, (plan.rows, 2 * cap), 1).astype(jnp.float32)

        @pl.loop(0, hidden // tile)
        def _(step):
            cols = pl.ds(pl.multiple_of(step * tile, tile), tile)
            for yy in range(2):
                rows = pl.ds(pl.multiple_of((4 * p + 2 * yy) * cap, 2 * cap), 2 * cap)
                values = view[1, 0, rows, cols].astype(jnp.float32)
                normal_cdf = 0.5 * (1.0 + lax.erf(values * root_half))
                density = inv_root_two_pi * jnp.exp(-0.5 * values * values)
                steep = normal_cdf + values * density
                active = (values * normal_cdf).astype(jnp.bfloat16)
                high = steep.astype(jnp.bfloat16)
                low = (steep - high.astype(jnp.float32)).astype(jnp.bfloat16)
                for cc in range(2):
                    j = 2 * cc + yy
                    sel = jnp.where(turned[:, j : j + 1] + float(cc * cap) == spot, 1.0, 0.0)
                    sel = sel.astype(jnp.bfloat16)
                    gate = turned[:, 4 + j : 5 + j]
                    pick = lambda rhs: jnp.dot(sel, rhs, preferred_element_type=jnp.float32)
                    steeps = (pick(high) + pick(low)) * gate
                    actives = (pick(active) * gate).astype(jnp.bfloat16)
                    for chain in range(chains):
                        to = pl.ds(pl.multiple_of((4 * p + j) * n, n), n)
                        slope[chain, to, cols] = steeps[chain * n : (chain + 1) * n]
                        act[chain, to, cols] = actives[chain * n : (chain + 1) * n]

    unit_rows = 4 * n

    def apply(f, chain, i):
        p = plane_at(i)
        rows = pl.ds(pl.multiple_of(p * unit_rows, unit_rows), unit_rows)
        if i == 0:
            drain(("rs", chain))

        @pl.loop(0, hidden // tile)
        def _(step):
            cols = pl.ds(pl.multiple_of(step * tile, tile), tile)
            inner = jnp.dot(
                view[f % 2, chain, rows, :], down[:, cols], preferred_element_type=jnp.float32
            )
            scaled[:, cols] = (inner * slope[chain, rows, cols]).astype(jnp.bfloat16)

        wide = 2 * tile

        @pl.loop(0, width // wide)
        def _(step):
            cols = pl.ds(pl.multiple_of(step * wide, wide), wide)
            piece = lax.dot_general(
                scaled[...],
                up[cols, :],
                (((1,), (1,)), ((), ())),
                preferred_element_type=jnp.float32,
            )
            part[chain, rows, cols] = piece.astype(jnp.bfloat16)

        away = pl.ds(pl.multiple_of(p * unit_rows + (1 - core) * 2 * n, 2 * n), 2 * n)
        post(
            ("rs", chain),
            None,
            ("gift", chain, i),
            part.at[chain, away],
            gift.at[chain, p],
            sib_peer,
        )

    def part_rows(p, yy):
        return pl.multiple_of(slot_of(p, yy, core) * n, n)

    chunk = 16

    def add_up(terms, store):
        @pl.loop(0, n // chunk)
        def _(step):
            start = pl.multiple_of(step * chunk, chunk)
            value = None
            for term in terms:
                x = term(start).astype(jnp.float32)
                value = x if value is None else value + x
            store(start, value)

    def from_part(chain, p, yy, cols):
        base = part_rows(p, yy)
        return lambda s: part[chain, pl.ds(pl.multiple_of(base + s, chunk), chunk), cols]

    def to_part(chain, p, yy, cols):
        base = part_rows(p, yy)

        def store(s, value):
            rows = pl.ds(pl.multiple_of(base + s, chunk), chunk)
            part[chain, rows, cols] = value.astype(jnp.bfloat16)

        return store

    def from_gift(chain, p, yy, cols):
        base = pl.multiple_of(yy * n, n)
        return lambda s: gift[chain, p, pl.ds(pl.multiple_of(base + s, chunk), chunk), cols]

    def rows_at(s):
        return pl.ds(s, chunk)

    def lend(chain, i):
        p = plane_at(i)
        arrive(None, ("gift", chain, i), gift.at[chain, p])
        add_up(
            [from_part(chain, p, 1 - y, full), from_gift(chain, p, 1 - y, full)],
            to_part(chain, p, 1 - y, full),
        )
        src = part.at[chain, pl.ds(part_rows(p, 1 - y), n), c1]
        post(("rs", chain), None, ("lend", chain, i), src, rung.at[chain, p], rung_peer)

    def lent(chain, i):
        arrive(None, ("lend", chain, i), rung.at[chain, plane_at(i)])

    def carry(chain, d):
        for way, peer in sources:
            to = z + d if way == 0 else z - d
            cond = there(1 - way, d)
            more = both(cond, has[way])

            @pl.when(cond)
            def _():
                group = ("rs", chain)
                if d + 1 < planes:
                    arrive(more, ("rs2", chain, way, d + 1), came2.at[chain, way, to])
                add_up(
                    [
                        from_part(chain, to, 1 - y, c2),
                        lambda s: came2[chain, way, to, rows_at(s), :],
                    ],
                    to_part(chain, to, 1 - y, c2),
                )
                src = part.at[chain, pl.ds(part_rows(to, 1 - y), n), c2]
                copy(("rs2", chain, way, d), src, came2.at[chain, way, to], peer).start()
                if d + 1 < planes:
                    arrive(more, ("rs", chain, way, d + 1), came.at[chain, way, to])
                add_up(
                    [
                        from_part(chain, to, y, c1),
                        from_gift(chain, to, y, c1),
                        lambda s: rung[chain, to, rows_at(s), :],
                        lambda s: came[chain, way, to, rows_at(s), c1],
                    ],
                    to_part(chain, to, y, c1),
                )
                add_up(
                    [
                        from_part(chain, to, y, c2),
                        from_gift(chain, to, y, c2),
                        lambda s: came[chain, way, to, rows_at(s), c2],
                    ],
                    to_part(chain, to, y, c2),
                )
                src = part.at[chain, pl.ds(part_rows(to, y), n)]
                copy(("rs", chain, way, d), src, came.at[chain, way, to], peer).start()

            group = ("rs", chain)
            src2 = part.at[chain, pl.ds(part_rows(to, 1 - y), n), c2]
            src1 = part.at[chain, pl.ds(part_rows(to, y), n)]
            pending.setdefault(group, []).append((cond, ("rs2", chain, way, d), src2, peer))
            pending.setdefault(group, []).append((cond, ("rs", chain, way, d), src1, peer))

    def settle2(chain):
        for way in range(2):
            arrive(has[way], ("rs2", chain, way, 1), came2.at[chain, way, z])
        add_up(
            [from_part(chain, z, 1 - y, c2)]
            + [lambda s, way=way: came2[chain, way, z, rows_at(s), :] for way in range(2)],
            to_part(chain, z, 1 - y, c2),
        )
        src = part.at[chain, pl.ds(part_rows(z, 1 - y), n), c2]
        post(("rs", chain), None, ("last", chain), src, last.at[chain], rung_peer)

    def settle(f, chain):
        for way in range(2):
            arrive(has[way], ("rs", chain, way, 1), came.at[chain, way, z])

        def finish(cols):
            def store(s, value):
                rows = pl.ds(pl.multiple_of(chain * n + s, chunk), chunk)
                term = value.astype(jnp.bfloat16)
                if f == 0:
                    first[rows, cols] = term
                else:
                    whole = (
                        cot[rows, cols].astype(jnp.float32)
                        + first[rows, cols].astype(jnp.float32)
                        + term.astype(jnp.float32)
                    )
                    grad_in[rows, cols] = whole.astype(jnp.bfloat16)

            return store

        sides = [lambda s, way=way: came[chain, way, z, rows_at(s), c1] for way in range(2)]
        add_up(
            [
                from_part(chain, z, y, c1),
                from_gift(chain, z, y, c1),
                lambda s: rung[chain, z, rows_at(s), :],
            ]
            + sides,
            finish(c1),
        )
        arrive(None, ("last", chain), last.at[chain])
        sides = [lambda s, way=way: came[chain, way, z, rows_at(s), c2] for way in range(2)]
        add_up(
            [
                from_part(chain, z, y, c2),
                from_gift(chain, z, y, c2),
                lambda s: last[chain, rows_at(s), :],
            ]
            + sides,
            finish(c2),
        )

    def swap(chain):
        rows = chain_rows(chain)
        away = pl.ds(pl.multiple_of((1 - token) * half, half), half)
        keep = pl.ds(pl.multiple_of(token * half, half), half)
        post(
            "swap",
            None,
            ("swap", chain),
            grad_in.at[rows, away],
            third.at[rows, pl.ds(half, half)],
            far_peer,
        )
        third[rows, pl.ds(0, half)] = grad_in[rows, keep]

    def swapped(chain):
        arrive(None, ("swap", chain), third.at[chain_rows(chain), pl.ds(half, half)])

    def weigh(chain, i, begin, end):
        p = plane_at(i)
        rows = pl.ds(pl.multiple_of(p * unit_rows, unit_rows), unit_rows)

        @pl.loop(0, half // tile)
        def _(step):
            base = pl.multiple_of(step * tile, tile)
            out = pl.ds(base, tile)
            dims = (((0,), (0,)), ((), ()))
            value = lax.dot_general(
                view[0, chain, rows, pl.ds(base, tile)],
                act[chain, rows, :],
                dims,
                preferred_element_type=jnp.float32,
            )
            value = value + lax.dot_general(
                view[0, chain, rows, pl.ds(pl.multiple_of(half + base, tile), tile)],
                other[chain, rows, :],
                dims,
                preferred_element_type=jnp.float32,
            )
            if not begin:
                value = value + total[out, :]
            if end:
                grad_w[out, :] = (value * grad_scale).astype(jnp.bfloat16)
            else:
                total[out, :] = value

    for load in loads:
        load.start()
    barrier = pltpu.get_barrier_semaphore()
    for cond, peer in (
        (has[1], up_peer),
        (has[0], down_peer),
        (None, rung_peer),
        (None, sib_peer),
        (None, far_peer),
    ):
        when(
            cond,
            lambda: pl.semaphore_signal(barrier, inc=1, device_id=peer, device_id_type=MESH),
        )
    make_table()
    turn[...] = jnp.zeros_like(turn)
    for way in range(2):

        @pl.when(jnp.logical_not(has[way]))
        def _():
            for chain in range(chains):
                came[chain, way] = jnp.zeros(came.shape[2:], came.dtype)
                came2[chain, way] = jnp.zeros(came2.shape[2:], came2.dtype)

    count = 3 + jnp.where(z > 0, 1, 0) + jnp.where(z < planes - 1, 1, 0)
    pl.semaphore_wait(barrier, count)

    last_step = planes - 1
    tab_start()
    start(0, 0)
    tab_step(0)
    for load in loads:
        load.wait()
    for d in range(planes):
        if d:
            tab_step(d)
            tab_across(d)
        hop(0, 0, d)
        tab_ready(d)
        prepare(d)
        over(0, 0, d)
        if d == 0:
            start(0, 1)
        apply(0, 0, d)
    post("act", None, "act", act, other, far_peer)

    def slot(f, a, g, b, begin, unit):
        if begin:
            begin()
        lend(b, last_step)
        for d in range(planes):
            hop(f, a, d)
            if d < last_step:
                lend(b, last_step - 1 - d)
                lent(b, last_step - d)
                carry(b, last_step - d)
            over(f, a, d)
            unit(a, d)
        lent(b, 0)
        settle2(b)
        settle(g, b)

    slot(0, 1, 0, 0, None, lambda a, i: apply(0, a, i))
    slot(1, 0, 0, 1, lambda: start(1, 0), lambda a, i: apply(1, a, i))
    slot(1, 1, 1, 0, lambda: start(1, 1), lambda a, i: apply(1, a, i))
    swap(0)
    arrive(None, "act", other)
    swapped(0)
    slot(2, 0, 1, 1, lambda: start(2, 0), lambda a, i: weigh(a, i, i == 0, False))
    swap(1)
    swapped(1)
    start(2, 1)
    for d in range(planes):
        hop(2, 1, d)
        over(2, 1, d)
        weigh(1, d, False, d == last_step)
    for group in list(pending):
        drain(group)


def fused(plan, cotangent, expert_ids, gate_values, hidden_pre, up_weight, down_weight):
    experts, planes, chains, n = plan.experts, plan.planes, plan.chains, plan.n
    width, hidden, rows = plan.width, plan.hidden, plan.rows
    half = width // 2
    low, dma = jnp.bfloat16, pltpu.SemaphoreType.DMA
    vmem = pl.BlockSpec(memory_space=pltpu.VMEM)
    hbm = pl.BlockSpec(memory_space=pl.ANY)
    count = plan.semaphores()
    return pl.pallas_call(
        functools.partial(fused_kernel, plan),
        out_shape=[
            jax.ShapeDtypeStruct((rows, width), low),
            jax.ShapeDtypeStruct((half, hidden), low),
        ],
        in_specs=[vmem, vmem, vmem, hbm, hbm, hbm],
        out_specs=[vmem, vmem],
        scratch_shapes=[
            pltpu.VMEM((2, chains, experts * n, width), low),
            pltpu.VMEM((chains, experts * n, width), low),
            pltpu.VMEM((chains, planes, 2 * n, width), low),
            pltpu.VMEM((chains, 2, planes, n, width), low),
            pltpu.VMEM((chains, 2, planes, n, width - plan.split), low),
            pltpu.VMEM((chains, planes, n, plan.split), low),
            pltpu.VMEM((chains, n, width - plan.split), low),
            pltpu.VMEM((chains, experts * n, hidden), jnp.float32),
            pltpu.VMEM((chains, experts * n, hidden), low),
            pltpu.VMEM((chains, experts * n, hidden), low),
            pltpu.VMEM((rows, width), low),
            pltpu.VMEM((rows, width), low),
            pltpu.VMEM((experts, 2 * experts, rows), jnp.float32),
            pltpu.VMEM((2 * experts, rows), jnp.float32),
            pltpu.VMEM((rows, rows), jnp.float32),
            pltpu.VMEM((4 * n, hidden), low),
            pltpu.VMEM((width, hidden), low),
            pltpu.VMEM((width, hidden), low),
            pltpu.VMEM((half, hidden), jnp.float32),
            dma((count,)),
            dma((count,)),
            dma((3,)),
        ],
        compiler_params=pltpu.CompilerParams(
            collective_id=5, has_side_effects=True, vmem_limit_bytes=67_043_328
        ),
        cost_estimate=pl.CostEstimate(
            flops=40_000_000_000, bytes_accessed=20_000_000, transcendentals=0
        ),
        name="fused",
    )(cotangent, expert_ids, gate_values, hidden_pre, up_weight, down_weight)


def body(cotangent, expert_ids, gate_values, hidden_pre, up_weight, down_weight):
    plan = Plan(
        lax.axis_size("expert"),
        lax.axis_size("token"),
        cotangent.shape[0],
        cotangent.shape[1],
        hidden_pre.shape[2],
        hidden_pre.shape[1],
    )
    if not plan.fits():
        return staged(cotangent, expert_ids, gate_values, hidden_pre, up_weight, down_weight)
    input_grad, grad_out = fused(
        plan, cotangent, expert_ids, gate_values, hidden_pre[0], up_weight[0], down_weight[0]
    )
    return (input_grad, grad_out[None])


def solution(mesh):
    in_specs = (
        P(("expert", "token"), None),
        P(("expert", "token"), None),
        P(("expert", "token"), None),
        P("expert", "token", None),
        P("expert", None, None),
        P("expert", None, None),
    )
    out_specs = (P(("expert", "token"), None), P("expert", "token", None))
    return jax.shard_map(body, mesh=mesh, in_specs=in_specs, out_specs=out_specs, check_vma=False)
```

```python
import functools

import jax
import jax.numpy as jnp
from jax import lax
from jax.experimental import pallas as pl
from jax.experimental.pallas import tpu as pltpu
from jax.sharding import PartitionSpec as P

grad_scale = 0.03125
root_half = 0.7071067811865476
inv_root_two_pi = 0.3989422804014327


def slope_and_act(hidden_rows):
    values = hidden_rows.astype(jnp.float32)
    normal_cdf = 0.5 * (1.0 + lax.erf(values * root_half))
    density = inv_root_two_pi * jnp.exp(-0.5 * values * values)
    slopes = normal_cdf + values * density
    active = (values * normal_cdf).astype(jnp.bfloat16)
    return (slopes, active)


def slot_tables(ids, gates, capacity):
    me = lax.axis_index("expert")
    hit = ids == me
    match = jnp.any(hit, axis=2)
    gate = jnp.sum(jnp.where(hit, gates, 0.0), axis=2)
    rows = ids.shape[1]
    order = jnp.arange(rows, dtype=jnp.int32)
    before = (order[:, None] < order[None, :]).astype(jnp.bfloat16)
    rank = jnp.dot(match.astype(jnp.bfloat16), before, preferred_element_type=jnp.float32)
    rank = jnp.where(match, rank.astype(jnp.int32), -1)
    chosen = rank[:, None, :] == jnp.arange(capacity, dtype=jnp.int32)[None, :, None]
    slot_gate = jnp.sum(jnp.where(chosen, gate[:, None, :], 0.0), axis=2)
    return chosen.astype(jnp.bfloat16), slot_gate


MESH = pl.DeviceIdType.MESH


def ring_place(experts):
    chips = experts // 2
    side = chips // 2
    me = lax.axis_index("expert")
    core = me % 2
    chip = me // 2
    row, odd = chip // 2, chip % 2
    place = row + odd * (chips - 1 - 2 * row)

    def device(at):
        at = (at + 2 * chips) % chips
        back = at // side
        return ((at + back * (chips - 1 - 2 * at)) * 2 + back) * 2

    return place, core, device


def ring_messages(chips):
    side = chips // 2
    return [
        [(d, h) for d in range(1, side + 1) for h in range(2) if d < side or h == way]
        for way in range(2)
    ]


def greet(peers):
    barrier = pltpu.get_barrier_semaphore()
    for peer in peers:
        pl.semaphore_signal(barrier, inc=1, device_id={"expert": peer}, device_id_type=MESH)
    pl.semaphore_wait(barrier, len(peers))


def send(src, dst, send_sem, recv_sem, peer):
    return pltpu.make_async_remote_copy(
        src_ref=src,
        dst_ref=dst,
        send_sem=send_sem,
        recv_sem=recv_sem,
        device_id={"expert": peer},
        device_id_type=MESH,
    )


def gather_kernel(experts, count, *refs):
    mine, outs = refs[:count], refs[count : 2 * count]
    hop_send, hop_recv, sib_send, sib_recv, own_sem, cross_sems = refs[2 * count :]
    chips = experts // 2
    messages = ring_messages(chips)
    place, core, device = ring_place(experts)
    me = lax.axis_index("expert")
    sibling = me + 1 - 2 * core
    peers = (device(place + 1) + core, device(place - 1) + core)
    own = [pltpu.make_async_copy(mine[i], outs[i].at[me], own_sem.at[i]) for i in range(count)]
    for copy in own:
        copy.start()
    greet(peers + (sibling,))

    def rows_of(i, half):
        size = mine[i].shape[0] // 2
        return pl.ds(half * size, size)

    def hop(i, way, index):
        distance, half = messages[way][index]
        sign = 1 - 2 * way
        rows = rows_of(i, half)
        origin = device(place - sign * (distance - 1)) + core
        src = mine[i].at[rows] if distance == 1 else outs[i].at[origin, rows]
        return send(
            src,
            outs[i].at[origin, rows],
            hop_send.at[i, way, index],
            hop_recv.at[i, way, index],
            peers[way],
        )

    def landed(i, way, index, which):
        distance, half = messages[way][index]
        origin = device(place - (1 - 2 * way) * distance) + which
        return outs[i].at[origin, rows_of(i, half)]

    def across(i, way, index, which):
        block = landed(i, way, index, which)
        return send(
            block, block, sib_send.at[i, way, index], sib_recv.at[i, way, index], sibling
        )

    for index in range(2):
        for way in range(2):
            for i in range(count):
                if index < len(messages[way]) and messages[way][index][0] == 1:
                    hop(i, way, index).start()
    cross = [
        send(mine[i], outs[i].at[me], cross_sems.at[0, i], cross_sems.at[1, i], sibling)
        for i in range(count)
    ]
    for copy in cross:
        copy.start()
    for index in range(len(messages[0])):
        for way in range(2):
            distance, half = messages[way][index]
            for i in range(count):
                block = landed(i, way, index, core)
                send(
                    block,
                    block,
                    hop_send.at[i, way, index],
                    hop_recv.at[i, way, index],
                    peers[way],
                ).wait_recv()
                if (distance + 1, half) in messages[way]:
                    hop(i, way, messages[way].index((distance + 1, half))).start()
                across(i, way, index, core).start()
    for i in range(count):
        own[i].wait()
        cross[i].wait_send()
        send(
            mine[i], outs[i].at[sibling], cross_sems.at[0, i], cross_sems.at[1, i], sibling
        ).wait_recv()
        for way in range(2):
            for index in range(len(messages[way])):
                hop(i, way, index).wait_send()
                across(i, way, index, core).wait_send()
                across(i, way, index, 1 - core).wait_recv()


def gather_rows(arrays, name):
    experts = lax.axis_size("expert")
    count = len(arrays)
    steps = len(ring_messages(experts // 2)[0])
    dma = pltpu.SemaphoreType.DMA
    return pl.pallas_call(
        functools.partial(gather_kernel, experts, count),
        out_shape=[jax.ShapeDtypeStruct((experts,) + a.shape, a.dtype) for a in arrays],
        in_specs=[pl.BlockSpec(memory_space=pltpu.VMEM)] * count,
        out_specs=[pl.BlockSpec(memory_space=pl.ANY)] * count,
        scratch_shapes=[
            dma((count, 2, steps)),
            dma((count, 2, steps)),
            dma((count, 2, steps)),
            dma((count, 2, steps)),
            dma((count,)),
            dma((2, count)),
        ],
        compiler_params=pltpu.CompilerParams(
            collective_id=name, has_side_effects=True, vmem_limit_bytes=8 * 1024 * 1024
        ),
        cost_estimate=pl.CostEstimate(
            flops=20_000_000_000, bytes_accessed=20_000_000, transcendentals=0
        ),
        name="gather" + str(name),
    )(*arrays)


def scatter_kernel(
    experts, parts, out, own, other, came, own_sem, sib_send, sib_recv, hop_send, hop_recv
):
    chips = experts // 2
    side = chips // 2
    messages = ring_messages(chips)
    place, core, device = ring_place(experts)
    me = lax.axis_index("expert")
    sibling = me + 1 - 2 * core
    peers = (device(place + 1) + core, device(place - 1) + core)
    size = out.shape[0] // 2
    order = [side]
    for d in range(side - 1, 0, -1):
        order += [d, chips - d]
    order += [0]
    loads = {
        k: pltpu.make_async_copy(parts.at[device(place + k) + core], own.at[k], own_sem.at[k])
        for k in order
    }
    for k in order:
        loads[k].start()
    greet(peers + (sibling,))
    gifts = {
        k: send(
            parts.at[device(place + k) + 1 - core],
            other.at[k],
            sib_send.at[k],
            sib_recv.at[k],
            sibling,
        )
        for k in order
    }
    for k in order:
        gifts[k].start()

    def hop(way, message):
        distance, half = message
        k = distance if way == 0 else chips - distance
        rows = pl.ds(half * size, size)
        index = messages[way].index(message)
        return send(
            own.at[k, rows],
            came.at[way, distance - 1, rows],
            hop_send.at[way, index],
            hop_recv.at[way, index],
            peers[way],
        )

    step = 16

    def add_up(k, half, more, target):
        @pl.loop(0, size // step)
        def _(at):
            rows = pl.ds(pl.multiple_of(half * size + at * step, step), step)
            total = own[k, rows, :].astype(jnp.float32) + other[k, rows, :].astype(jnp.float32)
            for way, slot in more:
                total = total + came[way, slot, rows, :].astype(jnp.float32)
            if target is None:
                own[k, rows, :] = total.astype(own.dtype)
            else:
                target[rows, :] = total.astype(target.dtype)

    ready = set()

    def get(k):
        if k not in ready:
            ready.add(k)
            loads[k].wait()
            gifts[k].wait_recv()

    for distance in range(side, 0, -1):
        for half in range(2):
            for way in range(2):
                if (distance, half) not in messages[way]:
                    continue
                k = distance if way == 0 else chips - distance
                get(k)
                more = []
                if (distance + 1, half) in messages[way]:
                    hop(way, (distance + 1, half)).wait_recv()
                    more = [(way, distance)]
                add_up(k, half, more, None)
                hop(way, (distance, half)).start()
    get(0)
    for half in range(2):
        more = []
        for way in range(2):
            if (1, half) in messages[way]:
                hop(way, (1, half)).wait_recv()
                more.append((way, 0))
        add_up(0, half, more, out)
    for k in order:
        gifts[k].wait_send()
    for way in range(2):
        for message in messages[way]:
            hop(way, message).wait_send()


def scatter_sum(blocks):
    experts, rows, width = blocks.shape
    chips = experts // 2
    steps = len(ring_messages(chips)[0])
    dma = pltpu.SemaphoreType.DMA
    buffers = (3 * chips + 4) * rows * width * 2
    return pl.pallas_call(
        functools.partial(scatter_kernel, experts),
        out_shape=jax.ShapeDtypeStruct((rows, width), blocks.dtype),
        in_specs=[pl.BlockSpec(memory_space=pl.ANY)],
        out_specs=pl.BlockSpec(memory_space=pltpu.VMEM),
        scratch_shapes=[
            pltpu.VMEM((chips, rows, width), blocks.dtype),
            pltpu.VMEM((chips, rows, width), blocks.dtype),
            pltpu.VMEM((2, chips // 2, rows, width), blocks.dtype),
            dma((chips,)),
            dma((chips,)),
            dma((chips,)),
            dma((2, steps)),
            dma((2, steps)),
        ],
        compiler_params=pltpu.CompilerParams(
            collective_id=7, has_side_effects=True, vmem_limit_bytes=buffers + 2 * 1024 * 1024
        ),
        cost_estimate=pl.CostEstimate(
            flops=20_000_000_000, bytes_accessed=20_000_000, transcendentals=0
        ),
        name="scatter_sum",
    )(blocks)


def from_groups(make):
    groups = lax.axis_size("token")
    mine = lax.axis_index("token")
    taken = [make(mine)]
    for shift in range(1, groups):
        pairs = [(t, (t + shift) % groups) for t in range(groups)]
        taken.append(lax.ppermute(make((mine + shift) % groups), "token", pairs))
    return jnp.stack(taken)


def pick(sel, rows):
    return lax.dot_general(
        sel, rows, (((2,), (1,)), ((0,), (0,))), preferred_element_type=jnp.float32
    ).astype(jnp.bfloat16)


def transpose_jacobian(everyone, sel, slot_gate, slopes, up_weight, down_weight):
    blocks, capacity, rows = sel.shape
    picked = pick(sel, everyone).reshape(blocks * capacity, -1)
    inner_prod = jnp.dot(picked, down_weight, preferred_element_type=jnp.float32)
    scaled = (inner_prod * slopes).astype(jnp.bfloat16)
    pieces = lax.dot_general(
        scaled, up_weight, (((1,), (1,)), ((), ())), preferred_element_type=jnp.float32
    ).astype(jnp.bfloat16)
    weighted = (pieces.astype(jnp.float32) * slot_gate.reshape(-1, 1)).astype(jnp.bfloat16)
    spread = lax.dot_general(
        sel,
        weighted.reshape(blocks, capacity, -1),
        (((1,), (1,)), ((0,), (0,))),
        preferred_element_type=jnp.float32,
    ).astype(jnp.bfloat16)
    return scatter_sum(spread)


def staged(cotangent, expert_ids, gate_values, hidden_pre, up_weight, down_weight):
    experts = lax.axis_size("expert")
    groups = lax.axis_size("token")
    rows, width = cotangent.shape
    top = expert_ids.shape[1]
    padded = -(-2 * top // 16) * 16
    routes = jnp.concatenate([expert_ids.T.astype(jnp.float32), gate_values.T], axis=0)
    routes = jnp.pad(routes, ((0, padded - 2 * top), (0, 0)))
    routes = from_groups(lambda group: routes).reshape(groups * padded, rows)
    everyone, all_routes = gather_rows([cotangent, routes], 1)
    slopes, active = slope_and_act(hidden_pre[0])
    capacity = slopes.shape[0] // experts
    acts = from_groups(lambda group: active)
    all_routes = all_routes.reshape(experts * groups, padded, rows).transpose(0, 2, 1)
    all_sel, all_gate = slot_tables(
        all_routes[:, :, :top].astype(jnp.int32), all_routes[:, :, top : 2 * top], capacity
    )
    by_group = all_sel.reshape(experts, groups, capacity, rows)
    sel = by_group[:, 0]
    slot_gate = all_gate.reshape(experts, groups, capacity)[:, 0]
    first_term = transpose_jacobian(
        everyone, sel, slot_gate, slopes, up_weight[0], down_weight[0]
    )
    (everyone,) = gather_rows([first_term], 2)
    second = transpose_jacobian(everyone, sel, slot_gate, slopes, up_weight[0], down_weight[0])
    input_grad = (
        cotangent.astype(jnp.float32) + first_term.astype(jnp.float32) + second.astype(jnp.float32)
    ).astype(jnp.bfloat16)
    share = width // groups
    columns = from_groups(
        lambda group: lax.dynamic_slice_in_dim(input_grad, group * share, share, 1)
    ).reshape(groups * rows, share)
    (everyone,) = gather_rows([columns], 3)
    everyone = everyone.reshape(experts * groups, rows, share)
    picked = pick(all_sel, everyone)
    routed = (picked.astype(jnp.float32) * all_gate[:, :, None]).astype(jnp.bfloat16)
    acts = acts.reshape(groups, experts, capacity, -1).transpose(1, 0, 2, 3)
    summed = lax.dot_general(
        routed.reshape(experts * groups * capacity, -1),
        acts.reshape(experts * groups * capacity, -1),
        (((0,), (0,)), ((), ())),
        preferred_element_type=jnp.float32,
    )
    grad_out = (summed * grad_scale).astype(jnp.bfloat16)[None]
    return (input_grad, grad_out)


NAMES = ("aS", "aH0", "aH", "aK", "aO", "aR", "tS", "tH0", "tH", "tO", "tR")
NAMES += ("P", "X", "N", "U", "L", "D", "C", "T2", "T1", "T", "W")
ORDER = (
    (6, 0, 0), (0, 0, 0), (0, 0, 1), (8, 0, 0, 1, 0), (1, 0, 0), (8, 0, 0, 1, 1), (2, 0, 0, 1, 0),
    (2, 0, 0, 1, 1), (8, 0, 0, 2, 0), (12, 0), (7, 0, 0), (8, 0, 0, 2, 1), (2, 0, 1, 1, 0),
    (2, 0, 1, 1, 1), (2, 0, 0, 2, 1), (3, 0, 0, 1, 1), (10, 0, 0, 0), (9, 0, 0, 1, 1),
    (9, 0, 0, 1, 0), (2, 0, 0, 2, 0), (11, 0), (10, 0, 0, 1), (1, 0, 1), (12, 1), (9, 0, 0, 2, 1),
    (3, 0, 0, 1, 0), (8, 0, 0, 3, 1), (9, 0, 0, 2, 0), (8, 0, 0, 3, 0), (0, 0, 3),
    (9, 0, 0, 3, 1), (4, 0, 0, 1, 0), (2, 0, 0, 3, 1), (10, 0, 0, 2), (11, 1), (3, 0, 0, 2, 1),
    (9, 0, 0, 3, 0), (4, 0, 1, 1, 0), (2, 0, 0, 3, 0), (3, 0, 0, 2, 0), (4, 0, 1, 1, 1),
    (2, 0, 1, 2, 1), (12, 2), (2, 0, 1, 2, 0), (4, 0, 0, 2, 1), (3, 0, 1, 1, 1), (5, 0, 0, 0),
    (10, 0, 0, 3), (3, 0, 1, 1, 0), (12, 3), (4, 0, 0, 2, 0), (4, 0, 0, 1, 1), (0, 0, 2), (11, 2),
    (11, 3), (4, 0, 0, 3, 1), (2, 0, 3, 1, 0), (5, 0, 0, 1), (4, 0, 0, 3, 0), (3, 0, 0, 3, 0),
    (2, 0, 3, 1, 1), (3, 0, 0, 3, 1), (14, 0, 0, 0), (14, 0, 0, 1), (5, 0, 0, 2), (5, 0, 1, 0),
    (5, 0, 1, 1), (5, 0, 0, 3), (2, 0, 1, 3, 0), (14, 0, 0, 2), (14, 0, 1, 0), (2, 0, 1, 3, 1),
    (14, 0, 0, 3), (3, 0, 1, 2, 1), (4, 0, 1, 2, 1), (3, 0, 1, 2, 0), (1, 0, 3), (15, 0, 0, 1),
    (4, 0, 1, 2, 0), (14, 0, 1, 1), (15, 0, 0, 3), (13,), (5, 0, 1, 2), (4, 0, 1, 3, 0),
    (4, 0, 1, 3, 1), (4, 0, 3, 1, 1), (16, 0, 0, 3, 1), (1, 0, 2), (16, 0, 0, 3, 0),
    (15, 0, 0, 2), (2, 0, 2, 1, 1), (3, 0, 1, 3, 0), (2, 0, 2, 1, 0), (14, 0, 1, 2),
    (2, 0, 3, 2, 1), (16, 0, 0, 2, 1), (3, 0, 1, 3, 1), (2, 0, 3, 2, 0), (16, 0, 0, 2, 0),
    (15, 0, 1, 1), (3, 0, 3, 1, 1), (5, 0, 3, 0), (5, 0, 1, 3), (3, 0, 3, 1, 0), (17, 0, 0, 3, 0),
    (17, 0, 0, 3, 1), (14, 0, 1, 3), (17, 0, 0, 2, 1), (3, 0, 2, 1, 1), (17, 0, 0, 2, 0),
    (15, 0, 1, 3), (16, 0, 0, 1, 0), (5, 0, 2, 0), (14, 0, 3, 0), (16, 0, 1, 3, 1),
    (2, 0, 2, 2, 1), (16, 0, 0, 1, 1), (2, 0, 3, 3, 0), (4, 0, 2, 1, 0), (4, 0, 3, 1, 0),
    (3, 0, 3, 2, 0), (15, 0, 1, 2), (2, 0, 3, 3, 1), (2, 0, 2, 2, 0), (4, 0, 2, 1, 1),
    (16, 0, 1, 3, 0), (16, 0, 1, 2, 1), (3, 0, 2, 1, 0), (16, 0, 1, 2, 0), (17, 0, 1, 3, 1),
    (4, 0, 3, 2, 1), (5, 0, 3, 1), (17, 0, 1, 3, 0), (4, 0, 3, 3, 0), (3, 0, 3, 2, 1),
    (17, 0, 0, 1, 0), (17, 0, 0, 1, 1), (4, 0, 3, 2, 0), (15, 0, 0, 0), (14, 0, 3, 1), (18, 0, 0),
    (5, 0, 2, 1), (17, 0, 1, 2, 1), (4, 0, 3, 3, 1), (2, 0, 2, 3, 1), (5, 0, 3, 2),
    (16, 0, 1, 1, 1), (3, 0, 2, 2, 0), (17, 0, 1, 2, 0), (3, 0, 2, 2, 1), (15, 0, 1, 0),
    (14, 0, 3, 2), (16, 0, 1, 1, 0), (3, 0, 3, 3, 0), (14, 0, 2, 0), (2, 0, 2, 3, 0), (19, 0, 0),
    (20, 0, 0), (3, 0, 3, 3, 1), (0, 1, 0), (5, 0, 3, 3), (14, 0, 3, 3), (3, 0, 2, 3, 1),
    (15, 0, 3, 1), (17, 0, 1, 1, 1), (4, 0, 2, 2, 0), (17, 0, 1, 1, 0), (18, 0, 1), (1, 1, 0),
    (15, 0, 3, 3), (5, 1, 0, 0), (4, 0, 2, 2, 1), (2, 1, 0, 1, 0), (16, 0, 3, 3, 0),
    (2, 1, 0, 1, 1), (16, 0, 3, 3, 1), (3, 0, 2, 3, 0), (19, 0, 1), (4, 0, 2, 3, 1), (20, 0, 1),
    (5, 0, 2, 2), (4, 0, 2, 3, 0), (0, 1, 1), (14, 0, 2, 1), (15, 0, 3, 2), (17, 0, 3, 3, 1),
    (4, 1, 0, 1, 0), (17, 0, 3, 3, 0), (3, 1, 0, 1, 1), (14, 0, 2, 2), (5, 0, 2, 3),
    (16, 0, 3, 2, 1), (2, 1, 0, 2, 1), (16, 0, 3, 2, 0), (3, 1, 0, 1, 0), (2, 1, 0, 2, 0),
    (14, 0, 2, 3), (2, 1, 1, 1, 1), (2, 1, 1, 1, 0), (1, 1, 1), (15, 0, 2, 3), (16, 0, 2, 3, 0),
    (16, 0, 3, 1, 1), (16, 0, 3, 1, 0), (16, 0, 2, 3, 1), (2, 1, 0, 3, 0), (3, 1, 0, 2, 1),
    (15, 0, 3, 0), (5, 1, 1, 0), (4, 1, 0, 2, 0), (15, 0, 2, 2), (2, 1, 0, 3, 1),
    (17, 0, 3, 2, 1), (4, 1, 0, 1, 1), (17, 0, 3, 2, 0), (2, 1, 1, 2, 1), (17, 0, 2, 3, 1),
    (3, 1, 0, 2, 0), (4, 1, 0, 3, 0), (3, 1, 1, 1, 0), (4, 1, 0, 2, 1), (14, 1, 0, 0),
    (17, 0, 2, 3, 0), (14, 1, 1, 0), (16, 0, 2, 2, 1), (5, 1, 0, 1), (2, 1, 1, 2, 0),
    (4, 1, 1, 1, 1), (14, 1, 0, 1), (15, 0, 2, 1), (18, 0, 3), (3, 1, 1, 1, 1), (15, 0, 2, 0),
    (5, 1, 0, 2), (16, 0, 2, 2, 0), (3, 1, 0, 3, 1), (17, 0, 3, 1, 0), (4, 1, 0, 3, 1),
    (14, 1, 0, 2), (17, 0, 3, 1, 1), (3, 1, 0, 3, 0), (17, 0, 2, 2, 1), (17, 0, 2, 2, 0),
    (5, 1, 0, 3), (16, 0, 2, 1, 0), (3, 1, 1, 2, 0), (3, 1, 1, 2, 1), (16, 0, 2, 1, 1),
    (4, 1, 1, 1, 0), (2, 1, 1, 3, 1), (2, 1, 1, 3, 0), (14, 1, 0, 3), (19, 0, 3), (20, 0, 3),
    (0, 1, 3), (3, 1, 1, 3, 1), (4, 1, 1, 3, 0), (17, 0, 2, 1, 1), (17, 0, 2, 1, 0),
    (4, 1, 1, 3, 1), (5, 1, 1, 1), (18, 0, 2), (3, 1, 1, 3, 0), (4, 1, 1, 2, 0), (4, 1, 1, 2, 1),
    (15, 1, 0, 3), (14, 1, 1, 1), (1, 1, 3), (5, 1, 1, 3), (16, 1, 0, 3, 1), (2, 1, 3, 1, 0),
    (5, 1, 1, 2), (16, 1, 0, 3, 0), (14, 1, 1, 2), (2, 1, 3, 1, 1), (14, 1, 1, 3), (19, 0, 2),
    (20, 0, 2), (0, 1, 2), (15, 1, 1, 3), (16, 1, 1, 3, 1), (16, 1, 1, 3, 0), (15, 1, 0, 2),
    (3, 1, 3, 1, 0), (17, 1, 0, 3, 0), (15, 1, 1, 2), (4, 1, 3, 1, 0), (16, 1, 0, 2, 1),
    (3, 1, 3, 1, 1), (17, 1, 0, 3, 1), (17, 1, 1, 3, 1), (4, 1, 3, 1, 1), (2, 1, 3, 2, 0),
    (5, 1, 3, 0), (2, 1, 3, 2, 1), (17, 1, 1, 3, 0), (1, 1, 2), (16, 1, 1, 2, 1), (5, 1, 3, 1),
    (14, 1, 3, 0), (16, 1, 0, 2, 0), (2, 1, 2, 1, 0), (16, 1, 1, 2, 0), (14, 1, 3, 1),
    (2, 1, 2, 1, 1), (2, 1, 3, 3, 0), (17, 1, 1, 2, 0), (2, 1, 3, 3, 1), (15, 1, 1, 1),
    (3, 1, 3, 2, 0), (17, 1, 1, 2, 1), (3, 1, 3, 2, 1), (4, 1, 3, 3, 1), (17, 1, 0, 2, 0),
    (15, 1, 0, 1), (16, 1, 1, 1, 0), (4, 1, 3, 2, 1), (16, 1, 0, 1, 0), (4, 1, 3, 2, 0),
    (4, 1, 3, 3, 0), (16, 1, 1, 1, 1), (3, 1, 3, 3, 0), (3, 1, 3, 3, 1), (2, 1, 2, 2, 1),
    (17, 1, 0, 2, 1), (16, 1, 0, 1, 1), (5, 1, 3, 2), (2, 1, 2, 2, 0), (14, 1, 3, 2),
    (5, 1, 3, 3), (17, 1, 1, 1, 1), (15, 1, 1, 0), (17, 1, 1, 1, 0), (15, 1, 0, 0),
    (3, 1, 2, 1, 1), (4, 1, 2, 1, 1), (14, 1, 3, 3), (18, 1, 1), (15, 1, 3, 3), (16, 1, 3, 3, 0),
    (16, 1, 3, 3, 1), (17, 1, 0, 1, 1), (2, 1, 2, 3, 1), (3, 1, 2, 1, 0), (18, 1, 0),
    (17, 1, 0, 1, 0), (19, 1, 1), (20, 1, 1), (15, 1, 3, 2), (16, 1, 3, 2, 1), (17, 1, 3, 3, 1),
    (3, 1, 2, 2, 0), (5, 1, 2, 0), (15, 1, 3, 1), (17, 1, 3, 3, 0), (3, 1, 2, 2, 1),
    (2, 1, 2, 3, 0), (16, 1, 3, 2, 0), (4, 1, 2, 1, 0), (21, 1), (14, 1, 2, 0), (4, 1, 2, 2, 0),
    (0, 2, 1), (5, 1, 2, 1), (4, 1, 2, 2, 1), (19, 1, 0), (20, 1, 0), (14, 1, 2, 1),
    (16, 1, 3, 1, 1), (17, 1, 3, 2, 0), (15, 1, 3, 0), (4, 1, 2, 3, 1), (16, 1, 3, 1, 0),
    (3, 1, 2, 3, 0), (4, 1, 2, 3, 0), (17, 1, 3, 2, 1), (5, 1, 2, 2), (3, 1, 2, 3, 1), (21, 0),
    (0, 2, 0), (14, 1, 2, 2), (5, 1, 2, 3), (14, 1, 2, 3), (2, 2, 1, 1, 0), (2, 2, 1, 1, 1),
    (17, 1, 3, 1, 0), (17, 1, 3, 1, 1), (15, 1, 2, 3), (16, 1, 2, 3, 1), (2, 2, 0, 1, 1),
    (1, 2, 1), (17, 1, 2, 3, 1), (2, 2, 0, 1, 0), (15, 1, 2, 2), (18, 1, 3), (16, 1, 2, 3, 0),
    (17, 1, 2, 3, 0), (15, 1, 2, 1), (5, 2, 1, 0), (16, 1, 2, 2, 1), (2, 2, 1, 2, 1),
    (15, 1, 2, 0), (16, 1, 2, 2, 0), (4, 2, 1, 1, 1), (1, 2, 0), (2, 2, 1, 2, 0), (19, 1, 3),
    (2, 2, 0, 2, 1), (17, 1, 2, 2, 1), (5, 2, 0, 0), (17, 1, 2, 2, 0), (3, 2, 1, 1, 1),
    (2, 2, 1, 3, 1), (3, 2, 1, 1, 0), (4, 2, 1, 1, 0), (2, 2, 0, 2, 0), (20, 1, 3),
    (4, 2, 0, 1, 1), (16, 1, 2, 1, 0), (3, 2, 0, 1, 1), (16, 1, 2, 1, 1), (3, 2, 0, 1, 0),
    (17, 1, 2, 1, 0), (17, 1, 2, 1, 1), (14, 2, 1, 0), (21, 3), (0, 2, 3), (2, 2, 0, 3, 0),
    (4, 2, 0, 1, 0), (18, 1, 2), (14, 2, 0, 0), (3, 2, 0, 2, 1), (4, 2, 1, 2, 0), (3, 2, 0, 2, 0),
    (2, 2, 0, 3, 1), (4, 2, 0, 2, 0), (3, 2, 1, 2, 1), (5, 2, 0, 1), (19, 1, 2), (4, 2, 0, 3, 0),
    (1, 2, 3), (20, 1, 2), (2, 2, 3, 1, 1), (3, 2, 0, 3, 0), (3, 2, 1, 2, 0), (2, 2, 3, 1, 0),
    (21, 2), (3, 2, 3, 1, 1), (4, 2, 0, 2, 1), (4, 2, 1, 3, 1), (0, 2, 2), (5, 2, 1, 1),
    (14, 2, 1, 1), (2, 2, 3, 2, 1), (5, 2, 0, 2), (14, 2, 0, 1), (3, 2, 3, 1, 0), (2, 2, 1, 3, 0),
    (3, 2, 1, 3, 1), (3, 2, 0, 3, 1), (4, 2, 1, 2, 1), (2, 2, 3, 2, 0), (4, 2, 3, 1, 1),
    (4, 2, 0, 3, 1), (5, 2, 3, 0), (2, 2, 2, 1, 1), (14, 2, 0, 2), (2, 2, 2, 1, 0),
    (4, 2, 3, 1, 0), (5, 2, 0, 3), (2, 2, 3, 3, 0), (1, 2, 2), (3, 2, 1, 3, 0), (14, 2, 3, 0),
    (5, 2, 3, 1), (4, 2, 1, 3, 0), (14, 2, 3, 1), (2, 2, 2, 2, 0), (2, 2, 3, 3, 1), (5, 2, 1, 3),
    (4, 2, 3, 2, 1), (5, 2, 1, 2), (3, 2, 3, 2, 0), (2, 2, 2, 2, 1), (14, 2, 0, 3),
    (2, 2, 2, 3, 1), (14, 2, 1, 2), (5, 2, 2, 0), (4, 2, 3, 3, 1), (3, 2, 2, 1, 1),
    (4, 2, 3, 2, 0), (3, 2, 2, 1, 0), (4, 2, 2, 1, 0), (4, 2, 2, 1, 1), (3, 2, 3, 2, 1),
    (4, 2, 3, 3, 0), (2, 2, 2, 3, 0), (14, 2, 2, 0), (14, 2, 1, 3), (3, 2, 3, 3, 0),
    (3, 2, 3, 3, 1), (5, 2, 2, 1), (5, 2, 3, 2), (3, 2, 2, 2, 1), (3, 2, 2, 2, 0), (14, 2, 2, 1),
    (14, 2, 3, 2), (5, 2, 3, 3), (4, 2, 2, 2, 0), (3, 2, 2, 3, 0), (4, 2, 2, 2, 1),
    (4, 2, 2, 3, 0), (4, 2, 2, 3, 1), (3, 2, 2, 3, 1), (14, 2, 3, 3), (5, 2, 2, 2), (5, 2, 2, 3),
    (14, 2, 2, 2), (14, 2, 2, 3),
)
ROUTE = ("S", "H0", "H", "K", "O", "R")
CHAINS = 1 + max(step[2] for step in ORDER if NAMES[step[0]] == "aS")
PLANES = 1 + max(step[3] for step in ORDER if NAMES[step[0]] == "U")
GATHER_SPLIT = ((13, 11, 10, 10), (9, 9, 9, 9), (10, 10, 11, 13))
SCATTER_SPLIT = ((10, 10, 10, 10), (10, 10, 10, 10))


class Plan:
    def __init__(self, experts, groups, rows, width, hidden, slots):
        self.experts, self.groups, self.rows, self.width = experts, groups, rows, width
        self.hidden, self.slots = hidden, slots
        self.capacity = slots // experts
        self.planes = experts // 4
        self.chains = CHAINS
        self.n = rows // self.chains
        self.gather_split = [[self.cut(c) for c in line] for line in GATHER_SPLIT]
        self.scatter_split = [[self.cut(c) for c in line] for line in SCATTER_SPLIT]
        self.lent = max(max(line) for line in self.scatter_split)
        self.rest = width - min(min(line) for line in self.scatter_split)

    def cut(self, sixteenths):
        return self.width * sixteenths // 16

    def fits(self):
        lanes = 128
        whole = (
            self.groups == 2
            and self.experts % 4 == 0
            and 2 * self.experts <= lanes
            and self.planes == PLANES
            and self.rows == lanes
            and self.n % 16 == 0
            and self.width % 2048 == 0
            and self.hidden % (2 * lanes) == 0
            and (2 * self.capacity) % 16 == 0
            and 2 * self.capacity <= 2 * lanes
            and max(self.slots, self.width) <= self.rows * self.experts
            and 2 * self.hidden <= self.width
        )
        return whole and self.bytes() <= 63 * 1024 * 1024

    def bytes(self):
        e, r, d, h, z = self.experts, self.rows, self.width, self.hidden, self.planes
        tokens = 2 * e * r * d * 2 + e * r * d * 2 + e * r * d
        lines = self.chains * self.n * (2 * z * (d + self.rest) + z * self.lent + self.rest) * 2
        return tokens + lines + 2 * d * h * 2 + e * r * h * (4 + 2 + 2) + 3 * r * d * 2 + d * h * 2 + d * h

    def semaphores(self):
        chain = ("rail", "rail2", "over", "sib", "gift", "lend", "sum", "sum2", "last", "swap")
        whole = sum(semaphores_of(self.planes, (kind,)) for kind in chain) * self.chains
        table = sum(semaphores_of(self.planes, (kind,)) for kind in ("rail", "over", "sib"))
        return whole + table + 1


def semaphores_of(planes, kind):
    sizes = {"rail": planes + 1, "rail2": planes + 1, "sum": planes + 1, "sum2": planes + 1}
    sizes.update(over=planes, sib=planes, gift=planes, lend=planes)
    return sizes.get(kind[0], 1)


def fused_kernel(
    plan,
    cot,
    ids,
    gates,
    hidden_hbm,
    up_hbm,
    down_hbm,
    grad_in_hbm,
    grad_w_hbm,
    grad_in,
    grad_w,
    view,
    part,
    gift,
    came,
    came2,
    rung,
    last,
    slope,
    act,
    first,
    third,
    tabs,
    own_tab,
    turn,
    scaled,
    up,
    down,
    total,
    send_sems,
    recv_sems,
    load_sems,
):
    experts, planes, chains, n = plan.experts, plan.planes, plan.chains, plan.n
    width, hidden, cap = plan.width, plan.hidden, plan.capacity
    top = ids.shape[0]
    span = experts * n
    half = width // 2
    me = lax.axis_index("expert")
    token = lax.axis_index("token")
    core = me % 2
    y = (me // 2) % 2
    z = me // 4
    has = {0: z > 0, 1: z < planes - 1}
    up_peer = {"expert": me + 4}
    down_peer = {"expert": me - 4}
    rung_peer = {"expert": me + 2 - 4 * y}
    sib_peer = {"expert": me + 1 - 2 * core}
    far_peer = {"token": 1 - token}
    sources = ((0, up_peer), (1, down_peer))
    full = pl.ds(0, width)

    def sides(split):
        return pl.ds(0, split), pl.ds(split, width - split)


    bases = {}

    def number(key):
        kind, at = key
        if kind not in bases:
            bases[kind] = sum(semaphores_of(planes, name) for name in bases)
        return bases[kind] + at

    def copy(key, src, dst, peer):
        at = number(key)
        return pltpu.make_async_remote_copy(
            src_ref=src,
            dst_ref=dst,
            send_sem=send_sems.at[at],
            recv_sem=recv_sems.at[at],
            device_id=peer,
            device_id_type=MESH,
        )

    def when(cond, action):
        if cond is None:
            action()
        else:
            pl.when(cond)(action)

    pending = {}

    def post(group, cond, key, src, dst, peer):
        when(cond, lambda: copy(key, src, dst, peer).start())
        if group is not None:
            owe(group, cond, key, src)

    def owe(group, cond, key, src):
        pending.setdefault(group, []).append((cond, key, src))

    def drain(group):
        for cond, key, src in pending.pop(group, []):
            when(cond, lambda: copy(key, src, src, sib_peer).wait_send())

    def arrive(cond, key, dst):
        when(cond, lambda: copy(key, dst, dst, sib_peer).wait_recv())

    def both(a, b):
        return b if a is None else (a if b is None else jnp.logical_and(a, b))

    def slot_of(p, yy, cc):
        return 4 * p + 2 * cc + yy

    def origin(way, d):
        return z - d if way == 0 else z + d

    def there(way, d):
        return z >= d if way == 0 else z + d < planes

    mine = slot_of(z, y, core)
    beside = slot_of(z, 1 - y, core)

    def gather(tag, at, src, split):
        group = ("ag", tag)
        whole = split is None
        c1, c2 = sides(width if whole else split)
        rail = lambda way, p: (("rail", tag), p + way)
        rail2 = lambda way, p: (("rail2", tag), p + way)
        across_key = lambda p: (("over", tag), p)
        sib = lambda p: (("sib", tag), p)

        def pair(p, cc):
            return at(slot_of(p, 0, cc), full, 2)

        def start():
            drain(group)
            post(group, None, across_key(z), src, at(mine, full), rung_peer)
            for way, peer in sources:
                post(group, has[1 - way], rail(way, z), src, at(mine, full), peer)
            post(None, None, sib(z), src, at(mine, full), sib_peer)
            owe(group, None, sib(z), pair(z, core))

        def meet():
            block = at(beside, full)
            arrive(None, across_key(z), block)
            if not whole:
                cut = at(beside, c2)
                for way, peer in sources:
                    post(group, has[1 - way], rail2(way, z), cut, cut, peer)
            post(None, None, sib(z), block, block, sib_peer)

        def hop(d, way):
            peer = sources[way][1]
            cond = there(way, d)
            p = origin(way, d)
            block = at(slot_of(p, y, core), full)
            arrive(cond, rail(way, p), block)
            if d + 1 < planes:
                post(group, both(cond, has[1 - way]), rail(way, p), block, block, peer)
            cut = block if whole else at(slot_of(p, y, core), c1)
            post(group, cond, across_key(p), cut, cut, rung_peer)
            post(None, cond, sib(p), block, block, sib_peer)
            owe(group, cond, sib(p), pair(p, core))

        def hop2(d, way):
            peer = sources[way][1]
            cond = there(way, d)
            p = origin(way, d)
            cut = at(slot_of(p, 1 - y, core), c2)
            arrive(cond, rail2(way, p), cut)
            if d + 1 < planes:
                post(group, both(cond, has[1 - way]), rail2(way, p), cut, cut, peer)
            post(None, cond, sib(p), cut, cut, sib_peer)

        def across(d, way):
            cond = there(way, d)
            p = origin(way, d)
            cut = at(slot_of(p, 1 - y, core), full if whole else c1)
            arrive(cond, across_key(p), cut)
            post(None, cond, sib(p), cut, cut, sib_peer)

        def ready(d):
            if d == 0:
                arrive(None, sib(z), pair(z, 1 - core))
                return
            for way in range(2):
                p = origin(way, d)
                arrive(there(way, d), sib(p), pair(p, 1 - core))

        return start, meet, hop, hop2, across, ready

    def plane_at(i):
        low = jnp.minimum(z, planes - 1 - z)
        near = jnp.where(z < planes // 2, 1, -1)
        d = jnp.where(i <= 2 * low, (i + 1) // 2, i - low)
        pair = jnp.where(z % 2 == 0, 1, -1)
        sign = jnp.where(i <= 2 * low, pair * (1 if i % 2 else -1), near)
        return z + sign * d if i else z

    tab_at = lambda slot, cols, count=0: tabs.at[pl.ds(slot, count) if count else slot]

    sources_of = {0: cot, 1: first, 2: third}

    def chain_rows(chain):
        return pl.ds(chain * n, n)

    stages = {}
    for chain in range(chains):
        for f in range(3):

            def at(slot, cols, count=1, f=f, chain=chain):
                rows = pl.ds(pl.multiple_of(chain * span + slot * n, n), count * n)
                return view.at[f % 2, rows, cols]

            src = sources_of[f].at[chain_rows(chain)]
            stages[f, chain] = gather(chain, at, src, plan.gather_split[f][chain])

    def start(f, chain):
        stages[f, chain][0]()
        rows = pl.ds(pl.multiple_of(chain * span + mine * n, n), n)
        view[f % 2, rows, :] = sources_of[f][chain_rows(chain), :]

    hidden_at = view.at[1, pl.ds(0, plan.slots), pl.ds(0, hidden)]
    up_at = view.at[1, pl.ds(0, width), pl.ds(hidden, hidden)]
    loads = [
        pltpu.make_async_copy(hidden_hbm, hidden_at, load_sems.at[0]),
        pltpu.make_async_copy(up_hbm, up_at, load_sems.at[1]),
        pltpu.make_async_copy(down_hbm, down, load_sems.at[2]),
    ]
    turns = 4

    def turn_up(k):
        size = width // turns
        if k == 0:
            loads[1].wait()
        up[:, k * size : (k + 1) * size] = view[
            1, k * size : (k + 1) * size, hidden : 2 * hidden
        ].T
        if k == turns - 1:
            loads[2].wait()

    def make_table():
        lanes = plan.rows
        kind = lax.broadcasted_iota(jnp.int32, (2 * experts, lanes), 0)
        lane = lax.broadcasted_iota(jnp.int32, (lanes, lanes), 1)
        row = lax.broadcasted_iota(jnp.int32, (lanes, lanes), 0)
        match = jnp.zeros(kind.shape, jnp.float32)
        gate = jnp.zeros(kind.shape, jnp.float32)
        for k in range(top):
            name = ids[k : k + 1, :]
            match = match + jnp.where(name == kind, 1.0, 0.0)
            gate = gate + jnp.where(name + experts == kind, gates[k : k + 1, :], 0.0)
        before = jnp.where(row < lane, 1.0, 0.0).astype(jnp.bfloat16)
        rank = jnp.dot(match.astype(jnp.bfloat16), before, preferred_element_type=jnp.float32)
        rank = jnp.where(match > 0.5, rank, -4.0 * lanes)
        table = jnp.where(kind < experts, rank, gate)
        own_tab[...] = table
        tabs[mine] = table

    tile = 256

    def prepare(i):
        p = plane_at(i)
        if i == 0:
            loads[0].wait()
            turn[...] = jnp.zeros_like(turn)
        for j in range(4):
            turn[pl.ds(j, 1), :] = tabs[4 * p + j, pl.ds(me, 1), :]
            turn[pl.ds(4 + j, 1), :] = tabs[4 * p + j, pl.ds(experts + me, 1), :]
        turned = turn[...].T
        spot = lax.broadcasted_iota(jnp.int32, (plan.rows, 2 * cap), 1).astype(jnp.float32)

        @pl.loop(0, hidden // tile)
        def _(step):
            cols = pl.ds(pl.multiple_of(step * tile, tile), tile)
            for yy in range(2):
                rows = pl.ds(pl.multiple_of((4 * p + 2 * yy) * cap, 2 * cap), 2 * cap)
                values = view[1, rows, cols].astype(jnp.float32)
                normal_cdf = 0.5 * (1.0 + lax.erf(values * root_half))
                density = inv_root_two_pi * jnp.exp(-0.5 * values * values)
                steep = normal_cdf + values * density
                active = (values * normal_cdf).astype(jnp.bfloat16)
                high = steep.astype(jnp.bfloat16)
                low = (steep - high.astype(jnp.float32)).astype(jnp.bfloat16)
                for cc in range(2):
                    j = 2 * cc + yy
                    sel = jnp.where(turned[:, j : j + 1] + float(cc * cap) == spot, 1.0, 0.0)
                    sel = sel.astype(jnp.bfloat16)
                    gate = turned[:, 4 + j : 5 + j]
                    pick = lambda rhs: jnp.dot(sel, rhs, preferred_element_type=jnp.float32)
                    steeps = (pick(high) + pick(low)) * gate
                    actives = (pick(active) * gate).astype(jnp.bfloat16)
                    for chain in range(chains):
                        cut = slice(chain * n, (chain + 1) * n)
                        to = pl.multiple_of(chain * span + (4 * p + j) * n, n)
                        slope[pl.ds(to, n), cols] = steeps[cut]
                        act[chain, p, 0, j * n : (j + 1) * n, cols] = actives[cut]

        if i == planes - 1:
            post("act", None, (("act",), 0), act.at[:, :, 0], act.at[:, :, 1], far_peer)

    unit_rows = 8 * n

    def pair_at(i):
        mine_first = z // 2 * 2
        return mine_first if i == 1 else planes - 2 - mine_first

    def apply(f, chain, i):
        if i % 2 == 0:
            return
        base = pl.multiple_of(chain * span + pair_at(i) * 4 * n, unit_rows)
        rows = pl.ds(base, unit_rows)
        if i == 1:
            drain(("rs", chain))
        inner = jnp.dot(view[f % 2, rows, :], down[...], preferred_element_type=jnp.float32)
        scaled[...] = (inner * slope[rows, :]).astype(jnp.bfloat16)
        wide = width // 2

        @pl.loop(0, width // wide)
        def _(step):
            cols = pl.ds(pl.multiple_of(step * wide, wide), wide)
            piece = jnp.dot(scaled[...], up[:, cols], preferred_element_type=jnp.float32)
            part[rows, cols] = piece.astype(jnp.bfloat16)

        for k in (i - 1, i):
            p = plane_at(k)
            away = pl.multiple_of(chain * span + p * 4 * n + (1 - core) * 2 * n, 2 * n)
            post(
                ("rs", chain),
                None,
                (("gift", chain), p),
                part.at[pl.ds(away, 2 * n)],
                gift.at[chain, p],
                sib_peer,
            )

    def part_rows(chain, p, yy):
        return pl.ds(pl.multiple_of(chain * span + slot_of(p, yy, core) * n, n), n)

    patch = 128

    def add_up(cols, terms, store):
        @pl.loop(0, cols.size // patch)
        def _(step):
            offset = pl.multiple_of(step * patch, patch)
            value = None
            for term, shift in terms:
                x = term(pl.ds(pl.multiple_of(offset + shift, patch), patch)).astype(jnp.float32)
                value = x if value is None else value + x
            store(pl.ds(pl.multiple_of(offset + cols.start, patch), patch), value)

    def from_part(chain, p, yy, cols):
        return (lambda at: part[part_rows(chain, p, yy), at]), cols.start

    def to_part(chain, p, yy):
        def store(at, value):
            part[part_rows(chain, p, yy), at] = value.astype(jnp.bfloat16)

        return store

    def from_gift(chain, p, yy, cols):
        rows = pl.ds(pl.multiple_of(yy * n, n), n)
        return (lambda at: gift[chain, p, rows, at]), cols.start

    def from_came(chain, way, p, cols):
        return (lambda at: came[chain, way, p, :, at]), cols.start

    def from_came2(chain, way, p):
        return (lambda at: came2[chain, way, p, :, at]), 0

    def lend(f, chain, i):
        p = plane_at(i)
        c1 = pl.ds(0, plan.scatter_split[f][chain])
        arrive(None, (("gift", chain), p), gift.at[chain, p])
        add_up(
            full,
            [from_part(chain, p, 1 - y, full), from_gift(chain, p, 1 - y, full)],
            to_part(chain, p, 1 - y),
        )
        src = part.at[part_rows(chain, p, 1 - y), c1]
        post(("rs", chain), None, (("lend", chain), p), src, rung.at[chain, p, :, c1], rung_peer)

    def lent(chain, p, c1):
        arrive(None, (("lend", chain), p), rung.at[chain, p, :, c1])

    def carry2(f, chain, d, way):
        c2 = sides(plan.scatter_split[f][chain])[1]
        place = came2.at[chain, way, :, :, pl.ds(0, c2.size)]
        peer = sources[way][1]
        to = z + d if way == 0 else z - d
        cond = there(1 - way, d)
        src = part.at[part_rows(chain, to, 1 - y), c2]

        @pl.when(cond)
        def _():
            if d + 1 < planes:
                arrive(has[way], (("sum2", chain), to + 1 - way), place.at[to])
            add_up(
                c2,
                [from_part(chain, to, 1 - y, c2), from_came2(chain, way, to)],
                to_part(chain, to, 1 - y),
            )
            copy((("sum2", chain), to + 1 - way), src, place.at[to], peer).start()

        owe(("rs", chain), cond, (("sum2", chain), to + 1 - way), src)

    def carry1(f, chain, d, way):
        c1, c2 = sides(plan.scatter_split[f][chain])
        peer = sources[way][1]
        to = z + d if way == 0 else z - d
        cond = there(1 - way, d)
        src = part.at[part_rows(chain, to, y)]

        @pl.when(cond)
        def _():
            lent(chain, to, c1)
            if d + 1 < planes:
                arrive(has[way], (("sum", chain), to + 1 - way), came.at[chain, way, to])
            for cols in (c1, c2):
                terms = [
                    from_part(chain, to, y, cols),
                    from_gift(chain, to, y, cols),
                    from_came(chain, way, to, cols),
                ]
                if cols is c1:
                    terms.append(((lambda at: rung[chain, to, :, at]), 0))
                add_up(cols, terms, to_part(chain, to, y))
            copy((("sum", chain), to + 1 - way), src, came.at[chain, way, to], peer).start()

        owe(("rs", chain), cond, (("sum", chain), to + 1 - way), src)

    def settle2(f, chain):
        c2 = sides(plan.scatter_split[f][chain])[1]
        short = pl.ds(0, c2.size)
        for way in range(2):
            arrive(has[way], (("sum2", chain), z + 1 - way), came2.at[chain, way, z, :, short])
        add_up(
            c2,
            [from_part(chain, z, 1 - y, c2)] + [from_came2(chain, w, z) for w in range(2)],
            to_part(chain, z, 1 - y),
        )
        src = part.at[part_rows(chain, z, 1 - y), c2]
        post(("rs", chain), None, (("last", chain), 0), src, last.at[chain, :, short], rung_peer)

    def finish(f, chain, cols, extra):
        rows = chain_rows(chain)

        def store(at, value):
            term = value.astype(jnp.bfloat16)
            if f == 0:
                first[rows, at] = term
            else:
                whole = (
                    cot[rows, at].astype(jnp.float32)
                    + first[rows, at].astype(jnp.float32)
                    + term.astype(jnp.float32)
                )
                grad_in[rows, at] = whole.astype(jnp.bfloat16)

        terms = [from_part(chain, z, y, cols), from_gift(chain, z, y, cols), extra]
        add_up(cols, terms + [from_came(chain, w, z, cols) for w in range(2)], store)

    def settle1(f, chain):
        c1 = pl.ds(0, plan.scatter_split[f][chain])
        lent(chain, z, c1)
        for way in range(2):
            arrive(has[way], (("sum", chain), z + 1 - way), came.at[chain, way, z])
        finish(f, chain, c1, ((lambda at: rung[chain, z, :, at]), 0))

    def settle(f, chain):
        c2 = sides(plan.scatter_split[f][chain])[1]
        arrive(None, (("last", chain), 0), last.at[chain, :, pl.ds(0, c2.size)])
        finish(f, chain, c2, ((lambda at: last[chain, :, at]), 0))
        if f == 1:
            swap(chain)
            rows = chain_rows(chain)
            save(chain, grad_in.at[rows], grad_in_hbm.at[rows])

    saved = []

    def save(at, src, dst):
        copy_out = pltpu.make_async_copy(src, dst, load_sems.at[at])
        copy_out.start()
        saved.append(copy_out)

    def swap(chain):
        rows = chain_rows(chain)
        away = pl.ds(pl.multiple_of((1 - token) * half, half), half)
        keep = pl.ds(pl.multiple_of(token * half, half), half)
        post(
            "swap",
            None,
            (("swap", chain), 0),
            grad_in.at[rows, away],
            third.at[rows, pl.ds(half, half)],
            far_peer,
        )
        third[rows, pl.ds(0, half)] = grad_in[rows, keep]

    def swapped(chain):
        arrive(None, (("swap", chain), 0), third.at[chain_rows(chain), pl.ds(half, half)])

    def weigh(chain, i, end):
        if i % 2 == 0:
            return
        p = pair_at(i)
        start = pl.multiple_of(chain * span + p * 4 * n, unit_rows)
        upper = pl.ds(start, 4 * n)
        lower = pl.ds(pl.multiple_of(start + 4 * n, 4 * n), 4 * n)

        @pl.loop(0, half // tile)
        def _(step):
            base = pl.multiple_of(step * tile, tile)
            out = pl.ds(base, tile)
            left = pl.ds(base, tile)
            right = pl.ds(pl.multiple_of(half + base, tile), tile)
            value = lax.dot_general(
                jnp.concatenate(
                    [view[0, rows, cols] for rows in (upper, lower) for cols in (left, right)],
                    axis=0,
                ),
                act[chain, pl.ds(p, 2)].reshape(2 * unit_rows, hidden),
                (((0,), (0,)), ((), ())),
                preferred_element_type=jnp.float32,
            )
            if end:
                grad_w[out, :] = ((total[out, :] + value) * grad_scale).astype(jnp.bfloat16)
                pltpu.make_async_copy(
                    grad_w.at[out], grad_w_hbm.at[out], load_sems.at[chains + step]
                ).start()
            else:
                total[out, :] += value

        if end:
            for step in range(half // tile):
                out = pl.ds(step * tile, tile)
                saved.append(
                    pltpu.make_async_copy(
                        grad_w.at[out], grad_w_hbm.at[out], load_sems.at[chains + step]
                    )
                )

    for load in loads:
        load.start()
    barrier = pltpu.get_barrier_semaphore()
    for cond, peer in (
        (has[1], up_peer),
        (has[0], down_peer),
        (None, rung_peer),
        (None, sib_peer),
        (None, far_peer),
    ):
        when(
            cond,
            lambda: pl.semaphore_signal(barrier, inc=1, device_id=peer, device_id_type=MESH),
        )
    make_table()
    count = 3 + jnp.where(z > 0, 1, 0) + jnp.where(z < planes - 1, 1, 0)
    pl.semaphore_wait(barrier, count)

    def clear():
        total[...] = jnp.zeros_like(total)
        for way in range(2):

            @pl.when(jnp.logical_not(has[way]))
            def _():
                for chain in range(chains):
                    came[chain, way] = jnp.zeros(came.shape[2:], came.dtype)
                    came2[chain, way] = jnp.zeros(came2.shape[2:], came2.dtype)

    units = [0]

    def unit(f, chain, i):
        if f < 2:
            apply(f, chain, i)
            return
        if units[0] == 0:
            arrive(None, (("act",), 0), act.at[:, :, 1])
        units[0] += 1
        weigh(chain, i, units[0] == chains * planes)

    tab = gather("tab", tab_at, own_tab, None)
    routes = {("a", f, c): stages[f, c] for f in range(3) for c in range(chains)}
    routes["t", 0, 0] = tab
    actions = {
        "P": prepare,
        "X": turn_up,
        "N": clear,
        "U": unit,
        "L": lend,
        "D": carry2,
        "C": carry1,
        "T2": settle2,
        "T1": settle1,
        "T": settle,
        "W": swapped,
        "aS": start,
        "tS": lambda f, c: tab[0](),
    }
    for kind, *args in ORDER:
        name = NAMES[kind]
        with jax.named_scope("_".join([name] + [str(a) for a in args])):
            if name in actions:
                actions[name](*args)
            else:
                routes[(name[0],) + tuple(args[:2])][ROUTE.index(name[1:])](*args[2:])
    for group in list(pending):
        drain(group)
    for copy_out in saved:
        copy_out.wait()


def fused(plan, cotangent, expert_ids, gate_values, hidden_pre, up_weight, down_weight):
    experts, planes, chains, n = plan.experts, plan.planes, plan.chains, plan.n
    width, hidden, rows = plan.width, plan.hidden, plan.rows
    half = width // 2
    low, dma = jnp.bfloat16, pltpu.SemaphoreType.DMA
    vmem = pl.BlockSpec(memory_space=pltpu.VMEM)
    hbm = pl.BlockSpec(memory_space=pl.ANY)
    count = plan.semaphores()
    return pl.pallas_call(
        functools.partial(fused_kernel, plan),
        out_shape=[
            jax.ShapeDtypeStruct((rows, width), low),
            jax.ShapeDtypeStruct((half, hidden), low),
        ],
        in_specs=[vmem, vmem, vmem, hbm, hbm, hbm],
        out_specs=[hbm, hbm],
        scratch_shapes=[
            pltpu.VMEM((rows, width), low),
            pltpu.VMEM((half, hidden), low),
            pltpu.VMEM((2, chains * experts * n, width), low),
            pltpu.VMEM((chains * experts * n, width), low),
            pltpu.VMEM((chains, planes, 2 * n, width), low),
            pltpu.VMEM((chains, 2, planes, n, width), low),
            pltpu.VMEM((chains, 2, planes, n, plan.rest), low),
            pltpu.VMEM((chains, planes, n, plan.lent), low),
            pltpu.VMEM((chains, n, plan.rest), low),
            pltpu.VMEM((chains * experts * n, hidden), jnp.float32),
            pltpu.VMEM((chains, planes, 2, 4 * n, hidden), low),
            pltpu.VMEM((rows, width), low),
            pltpu.VMEM((rows, width), low),
            pltpu.VMEM((experts, 2 * experts, rows), jnp.float32),
            pltpu.VMEM((2 * experts, rows), jnp.float32),
            pltpu.VMEM((rows, rows), jnp.float32),
            pltpu.VMEM((8 * n, hidden), low),
            pltpu.VMEM((hidden, width), low),
            pltpu.VMEM((width, hidden), low),
            pltpu.VMEM((half, hidden), jnp.float32),
            dma((count,)),
            dma((count,)),
            dma((max(3, chains + half // 256),)),
        ],
        compiler_params=pltpu.CompilerParams(
            collective_id=5, has_side_effects=True, vmem_limit_bytes=67_043_328
        ),
        cost_estimate=pl.CostEstimate(
            flops=40_000_000_000, bytes_accessed=20_000_000, transcendentals=0
        ),
        name="fused",
    )(cotangent, expert_ids.T, gate_values.T, hidden_pre, up_weight, down_weight)


def hand_on_kernel(count, pieces, *refs):
    sources, targets, held = refs[:count], refs[count : 2 * count], refs[2 * count : 3 * count]
    into, out = refs[3 * count :]
    loads, stores = [], []
    for i in range(count):
        size = sources[i].shape[0] // pieces
        for k in range(pieces):
            rows = pl.ds(k * size, size)
            at = i * pieces + k
            loads.append(
                pltpu.make_async_copy(sources[i].at[rows], held[i].at[rows], into.at[at])
            )
            stores.append(
                pltpu.make_async_copy(held[i].at[rows], targets[i].at[rows], out.at[at])
            )
    for load in loads:
        load.start()
    for load, store in zip(loads, stores):
        load.wait()
        store.start()
    for store in stores:
        store.wait()


def hand_on(arrays):
    count, pieces = len(arrays), 4
    place = pl.BlockSpec(memory_space=pl.ANY)
    dma = pltpu.SemaphoreType.DMA
    return pl.pallas_call(
        functools.partial(hand_on_kernel, count, pieces),
        out_shape=[jax.ShapeDtypeStruct(a.shape, a.dtype) for a in arrays],
        in_specs=[place] * count,
        out_specs=[place] * count,
        scratch_shapes=[pltpu.VMEM(a.shape, a.dtype) for a in arrays]
        + [dma((count * pieces,)), dma((count * pieces,))],
        name="hand_on",
    )(*arrays)


def body(cotangent, expert_ids, gate_values, hidden_pre, up_weight, down_weight):
    plan = Plan(
        lax.axis_size("expert"),
        lax.axis_size("token"),
        cotangent.shape[0],
        cotangent.shape[1],
        hidden_pre.shape[2],
        hidden_pre.shape[1],
    )
    if not plan.fits():
        return staged(cotangent, expert_ids, gate_values, hidden_pre, up_weight, down_weight)
    input_grad, grad_out = fused(
        plan, cotangent, expert_ids, gate_values, hidden_pre[0], up_weight[0], down_weight[0]
    )
    input_grad, grad_out = hand_on([input_grad, grad_out])
    return (input_grad, grad_out[None])


def solution(mesh):
    in_specs = (
        P(("expert", "token"), None),
        P(("expert", "token"), None),
        P(("expert", "token"), None),
        P("expert", "token", None),
        P("expert", None, None),
        P("expert", None, None),
    )
    out_specs = (P(("expert", "token"), None), P("expert", "token", None))
    return jax.shard_map(body, mesh=mesh, in_specs=in_specs, out_specs=out_specs, check_vma=False)
```

```python
import functools

import jax
import jax.numpy as jnp
from jax import lax
from jax.experimental import pallas as pl
from jax.experimental.pallas import tpu as pltpu
from jax.sharding import PartitionSpec as P

grad_scale = 0.03125
root_half = 0.7071067811865476
inv_root_two_pi = 0.3989422804014327


def slope_and_act(hidden_rows):
    values = hidden_rows.astype(jnp.float32)
    normal_cdf = 0.5 * (1.0 + lax.erf(values * root_half))
    density = inv_root_two_pi * jnp.exp(-0.5 * values * values)
    slopes = normal_cdf + values * density
    active = (values * normal_cdf).astype(jnp.bfloat16)
    return (slopes, active)


def slot_tables(ids, gates, capacity):
    me = lax.axis_index("expert")
    hit = ids == me
    match = jnp.any(hit, axis=2)
    gate = jnp.sum(jnp.where(hit, gates, 0.0), axis=2)
    rows = ids.shape[1]
    order = jnp.arange(rows, dtype=jnp.int32)
    before = (order[:, None] < order[None, :]).astype(jnp.bfloat16)
    rank = jnp.dot(match.astype(jnp.bfloat16), before, preferred_element_type=jnp.float32)
    rank = jnp.where(match, rank.astype(jnp.int32), -1)
    chosen = rank[:, None, :] == jnp.arange(capacity, dtype=jnp.int32)[None, :, None]
    slot_gate = jnp.sum(jnp.where(chosen, gate[:, None, :], 0.0), axis=2)
    return chosen.astype(jnp.bfloat16), slot_gate


MESH = pl.DeviceIdType.MESH


def ring_place(experts):
    chips = experts // 2
    side = chips // 2
    me = lax.axis_index("expert")
    core = me % 2
    chip = me // 2
    row, odd = chip // 2, chip % 2
    place = row + odd * (chips - 1 - 2 * row)

    def device(at):
        at = (at + 2 * chips) % chips
        back = at // side
        return ((at + back * (chips - 1 - 2 * at)) * 2 + back) * 2

    return place, core, device


def ring_messages(chips):
    side = chips // 2
    return [
        [(d, h) for d in range(1, side + 1) for h in range(2) if d < side or h == way]
        for way in range(2)
    ]


def greet(peers):
    barrier = pltpu.get_barrier_semaphore()
    for peer in peers:
        pl.semaphore_signal(barrier, inc=1, device_id={"expert": peer}, device_id_type=MESH)
    pl.semaphore_wait(barrier, len(peers))


def send(src, dst, send_sem, recv_sem, peer):
    return pltpu.make_async_remote_copy(
        src_ref=src,
        dst_ref=dst,
        send_sem=send_sem,
        recv_sem=recv_sem,
        device_id={"expert": peer},
        device_id_type=MESH,
    )


def gather_kernel(experts, count, *refs):
    mine, outs = refs[:count], refs[count : 2 * count]
    hop_send, hop_recv, sib_send, sib_recv, own_sem, cross_sems = refs[2 * count :]
    chips = experts // 2
    messages = ring_messages(chips)
    place, core, device = ring_place(experts)
    me = lax.axis_index("expert")
    sibling = me + 1 - 2 * core
    peers = (device(place + 1) + core, device(place - 1) + core)
    own = [pltpu.make_async_copy(mine[i], outs[i].at[me], own_sem.at[i]) for i in range(count)]
    for copy in own:
        copy.start()
    greet(peers + (sibling,))

    def rows_of(i, half):
        size = mine[i].shape[0] // 2
        return pl.ds(half * size, size)

    def hop(i, way, index):
        distance, half = messages[way][index]
        sign = 1 - 2 * way
        rows = rows_of(i, half)
        origin = device(place - sign * (distance - 1)) + core
        src = mine[i].at[rows] if distance == 1 else outs[i].at[origin, rows]
        return send(
            src,
            outs[i].at[origin, rows],
            hop_send.at[i, way, index],
            hop_recv.at[i, way, index],
            peers[way],
        )

    def landed(i, way, index, which):
        distance, half = messages[way][index]
        origin = device(place - (1 - 2 * way) * distance) + which
        return outs[i].at[origin, rows_of(i, half)]

    def across(i, way, index, which):
        block = landed(i, way, index, which)
        return send(
            block, block, sib_send.at[i, way, index], sib_recv.at[i, way, index], sibling
        )

    for index in range(2):
        for way in range(2):
            for i in range(count):
                if index < len(messages[way]) and messages[way][index][0] == 1:
                    hop(i, way, index).start()
    cross = [
        send(mine[i], outs[i].at[me], cross_sems.at[0, i], cross_sems.at[1, i], sibling)
        for i in range(count)
    ]
    for copy in cross:
        copy.start()
    for index in range(len(messages[0])):
        for way in range(2):
            distance, half = messages[way][index]
            for i in range(count):
                block = landed(i, way, index, core)
                send(
                    block,
                    block,
                    hop_send.at[i, way, index],
                    hop_recv.at[i, way, index],
                    peers[way],
                ).wait_recv()
                if (distance + 1, half) in messages[way]:
                    hop(i, way, messages[way].index((distance + 1, half))).start()
                across(i, way, index, core).start()
    for i in range(count):
        own[i].wait()
        cross[i].wait_send()
        send(
            mine[i], outs[i].at[sibling], cross_sems.at[0, i], cross_sems.at[1, i], sibling
        ).wait_recv()
        for way in range(2):
            for index in range(len(messages[way])):
                hop(i, way, index).wait_send()
                across(i, way, index, core).wait_send()
                across(i, way, index, 1 - core).wait_recv()


def gather_rows(arrays, name):
    experts = lax.axis_size("expert")
    count = len(arrays)
    steps = len(ring_messages(experts // 2)[0])
    dma = pltpu.SemaphoreType.DMA
    return pl.pallas_call(
        functools.partial(gather_kernel, experts, count),
        out_shape=[jax.ShapeDtypeStruct((experts,) + a.shape, a.dtype) for a in arrays],
        in_specs=[pl.BlockSpec(memory_space=pltpu.VMEM)] * count,
        out_specs=[pl.BlockSpec(memory_space=pl.ANY)] * count,
        scratch_shapes=[
            dma((count, 2, steps)),
            dma((count, 2, steps)),
            dma((count, 2, steps)),
            dma((count, 2, steps)),
            dma((count,)),
            dma((2, count)),
        ],
        compiler_params=pltpu.CompilerParams(
            collective_id=name, has_side_effects=True, vmem_limit_bytes=8 * 1024 * 1024
        ),
        cost_estimate=pl.CostEstimate(
            flops=20_000_000_000, bytes_accessed=20_000_000, transcendentals=0
        ),
        name="gather" + str(name),
    )(*arrays)


def scatter_kernel(
    experts, parts, out, own, other, came, own_sem, sib_send, sib_recv, hop_send, hop_recv
):
    chips = experts // 2
    side = chips // 2
    messages = ring_messages(chips)
    place, core, device = ring_place(experts)
    me = lax.axis_index("expert")
    sibling = me + 1 - 2 * core
    peers = (device(place + 1) + core, device(place - 1) + core)
    size = out.shape[0] // 2
    order = [side]
    for d in range(side - 1, 0, -1):
        order += [d, chips - d]
    order += [0]
    loads = {
        k: pltpu.make_async_copy(parts.at[device(place + k) + core], own.at[k], own_sem.at[k])
        for k in order
    }
    for k in order:
        loads[k].start()
    greet(peers + (sibling,))
    gifts = {
        k: send(
            parts.at[device(place + k) + 1 - core],
            other.at[k],
            sib_send.at[k],
            sib_recv.at[k],
            sibling,
        )
        for k in order
    }
    for k in order:
        gifts[k].start()

    def hop(way, message):
        distance, half = message
        k = distance if way == 0 else chips - distance
        rows = pl.ds(half * size, size)
        index = messages[way].index(message)
        return send(
            own.at[k, rows],
            came.at[way, distance - 1, rows],
            hop_send.at[way, index],
            hop_recv.at[way, index],
            peers[way],
        )

    step = 16

    def add_up(k, half, more, target):
        @pl.loop(0, size // step)
        def _(at):
            rows = pl.ds(pl.multiple_of(half * size + at * step, step), step)
            total = own[k, rows, :].astype(jnp.float32) + other[k, rows, :].astype(jnp.float32)
            for way, slot in more:
                total = total + came[way, slot, rows, :].astype(jnp.float32)
            if target is None:
                own[k, rows, :] = total.astype(own.dtype)
            else:
                target[rows, :] = total.astype(target.dtype)

    ready = set()

    def get(k):
        if k not in ready:
            ready.add(k)
            loads[k].wait()
            gifts[k].wait_recv()

    for distance in range(side, 0, -1):
        for half in range(2):
            for way in range(2):
                if (distance, half) not in messages[way]:
                    continue
                k = distance if way == 0 else chips - distance
                get(k)
                more = []
                if (distance + 1, half) in messages[way]:
                    hop(way, (distance + 1, half)).wait_recv()
                    more = [(way, distance)]
                add_up(k, half, more, None)
                hop(way, (distance, half)).start()
    get(0)
    for half in range(2):
        more = []
        for way in range(2):
            if (1, half) in messages[way]:
                hop(way, (1, half)).wait_recv()
                more.append((way, 0))
        add_up(0, half, more, out)
    for k in order:
        gifts[k].wait_send()
    for way in range(2):
        for message in messages[way]:
            hop(way, message).wait_send()


def scatter_sum(blocks):
    experts, rows, width = blocks.shape
    chips = experts // 2
    steps = len(ring_messages(chips)[0])
    dma = pltpu.SemaphoreType.DMA
    buffers = (3 * chips + 4) * rows * width * 2
    return pl.pallas_call(
        functools.partial(scatter_kernel, experts),
        out_shape=jax.ShapeDtypeStruct((rows, width), blocks.dtype),
        in_specs=[pl.BlockSpec(memory_space=pl.ANY)],
        out_specs=pl.BlockSpec(memory_space=pltpu.VMEM),
        scratch_shapes=[
            pltpu.VMEM((chips, rows, width), blocks.dtype),
            pltpu.VMEM((chips, rows, width), blocks.dtype),
            pltpu.VMEM((2, chips // 2, rows, width), blocks.dtype),
            dma((chips,)),
            dma((chips,)),
            dma((chips,)),
            dma((2, steps)),
            dma((2, steps)),
        ],
        compiler_params=pltpu.CompilerParams(
            collective_id=7, has_side_effects=True, vmem_limit_bytes=buffers + 2 * 1024 * 1024
        ),
        cost_estimate=pl.CostEstimate(
            flops=20_000_000_000, bytes_accessed=20_000_000, transcendentals=0
        ),
        name="scatter_sum",
    )(blocks)


def from_groups(make):
    groups = lax.axis_size("token")
    mine = lax.axis_index("token")
    taken = [make(mine)]
    for shift in range(1, groups):
        pairs = [(t, (t + shift) % groups) for t in range(groups)]
        taken.append(lax.ppermute(make((mine + shift) % groups), "token", pairs))
    return jnp.stack(taken)


def pick(sel, rows):
    return lax.dot_general(
        sel, rows, (((2,), (1,)), ((0,), (0,))), preferred_element_type=jnp.float32
    ).astype(jnp.bfloat16)


def transpose_jacobian(everyone, sel, slot_gate, slopes, up_weight, down_weight):
    blocks, capacity, rows = sel.shape
    picked = pick(sel, everyone).reshape(blocks * capacity, -1)
    inner_prod = jnp.dot(picked, down_weight, preferred_element_type=jnp.float32)
    scaled = (inner_prod * slopes).astype(jnp.bfloat16)
    pieces = lax.dot_general(
        scaled, up_weight, (((1,), (1,)), ((), ())), preferred_element_type=jnp.float32
    ).astype(jnp.bfloat16)
    weighted = (pieces.astype(jnp.float32) * slot_gate.reshape(-1, 1)).astype(jnp.bfloat16)
    spread = lax.dot_general(
        sel,
        weighted.reshape(blocks, capacity, -1),
        (((1,), (1,)), ((0,), (0,))),
        preferred_element_type=jnp.float32,
    ).astype(jnp.bfloat16)
    return scatter_sum(spread)


def staged(cotangent, expert_ids, gate_values, hidden_pre, up_weight, down_weight):
    experts = lax.axis_size("expert")
    groups = lax.axis_size("token")
    rows, width = cotangent.shape
    top = expert_ids.shape[1]
    padded = -(-2 * top // 16) * 16
    routes = jnp.concatenate([expert_ids.T.astype(jnp.float32), gate_values.T], axis=0)
    routes = jnp.pad(routes, ((0, padded - 2 * top), (0, 0)))
    routes = from_groups(lambda group: routes).reshape(groups * padded, rows)
    everyone, all_routes = gather_rows([cotangent, routes], 1)
    slopes, active = slope_and_act(hidden_pre[0])
    capacity = slopes.shape[0] // experts
    acts = from_groups(lambda group: active)
    all_routes = all_routes.reshape(experts * groups, padded, rows).transpose(0, 2, 1)
    all_sel, all_gate = slot_tables(
        all_routes[:, :, :top].astype(jnp.int32), all_routes[:, :, top : 2 * top], capacity
    )
    by_group = all_sel.reshape(experts, groups, capacity, rows)
    sel = by_group[:, 0]
    slot_gate = all_gate.reshape(experts, groups, capacity)[:, 0]
    first_term = transpose_jacobian(
        everyone, sel, slot_gate, slopes, up_weight[0], down_weight[0]
    )
    (everyone,) = gather_rows([first_term], 2)
    second = transpose_jacobian(everyone, sel, slot_gate, slopes, up_weight[0], down_weight[0])
    input_grad = (
        cotangent.astype(jnp.float32) + first_term.astype(jnp.float32) + second.astype(jnp.float32)
    ).astype(jnp.bfloat16)
    share = width // groups
    columns = from_groups(
        lambda group: lax.dynamic_slice_in_dim(input_grad, group * share, share, 1)
    ).reshape(groups * rows, share)
    (everyone,) = gather_rows([columns], 3)
    everyone = everyone.reshape(experts * groups, rows, share)
    picked = pick(all_sel, everyone)
    routed = (picked.astype(jnp.float32) * all_gate[:, :, None]).astype(jnp.bfloat16)
    acts = acts.reshape(groups, experts, capacity, -1).transpose(1, 0, 2, 3)
    summed = lax.dot_general(
        routed.reshape(experts * groups * capacity, -1),
        acts.reshape(experts * groups * capacity, -1),
        (((0,), (0,)), ((), ())),
        preferred_element_type=jnp.float32,
    )
    grad_out = (summed * grad_scale).astype(jnp.bfloat16)[None]
    return (input_grad, grad_out)


NAMES = ("aS", "aH0", "aH", "aK", "aO", "aR", "tS", "tH0", "tH", "tO", "tR")
NAMES += ("P", "X", "N", "U", "L", "D", "C", "T2", "T1", "T", "W")
ORDER = (
    (6, 0, 0), (13,), (0, 0, 0), (7, 0, 0), (0, 0, 1), (8, 0, 0, 1, 1), (12, 0), (8, 0, 0, 1, 0),
    (1, 0, 0), (2, 0, 0, 1, 0), (8, 0, 0, 2, 0), (2, 0, 0, 1, 1), (8, 0, 0, 2, 1), (12, 1),
    (12, 2), (2, 0, 1, 1, 1), (10, 0, 0, 0), (2, 0, 1, 1, 0), (3, 0, 0, 1, 0), (3, 0, 0, 1, 1),
    (1, 0, 1), (4, 0, 0, 1, 1), (9, 0, 0, 2, 0), (8, 0, 0, 3, 0), (9, 0, 0, 1, 0),
    (9, 0, 0, 2, 1), (9, 0, 0, 1, 1), (5, 0, 0, 0), (2, 0, 0, 2, 0), (8, 0, 0, 3, 1),
    (2, 0, 0, 2, 1), (2, 0, 1, 2, 1), (11, 0), (2, 0, 1, 2, 0), (3, 0, 0, 2, 1), (9, 0, 0, 3, 1),
    (3, 0, 0, 2, 0), (10, 0, 0, 1), (4, 0, 0, 1, 0), (12, 3), (5, 0, 1, 0), (0, 0, 2),
    (3, 0, 1, 1, 0), (11, 1), (4, 0, 0, 2, 0), (3, 0, 1, 1, 1), (4, 0, 0, 2, 1), (2, 0, 0, 3, 0),
    (4, 0, 1, 1, 1), (14, 0, 0, 0), (9, 0, 0, 3, 0), (10, 0, 0, 2), (5, 0, 0, 1), (2, 0, 0, 3, 1),
    (0, 0, 3), (4, 0, 1, 1, 0), (14, 0, 0, 1), (2, 0, 1, 3, 1), (11, 2), (3, 0, 0, 3, 0),
    (3, 0, 0, 3, 1), (2, 0, 1, 3, 0), (10, 0, 0, 3), (5, 0, 0, 2), (14, 0, 0, 2), (4, 0, 0, 3, 1),
    (4, 0, 0, 3, 0), (11, 3), (15, 0, 0, 1), (5, 0, 0, 3), (14, 0, 0, 3), (4, 0, 1, 2, 1),
    (3, 0, 1, 2, 1), (3, 0, 1, 2, 0), (4, 0, 1, 2, 0), (2, 0, 2, 1, 1), (2, 0, 2, 1, 0),
    (1, 0, 2), (2, 0, 3, 1, 0), (15, 0, 0, 3), (16, 0, 0, 3, 1), (4, 0, 1, 3, 1), (1, 0, 3),
    (14, 0, 1, 0), (5, 0, 1, 1), (3, 0, 1, 3, 1), (4, 0, 1, 3, 0), (5, 0, 1, 2), (16, 0, 0, 3, 0),
    (15, 0, 0, 2), (3, 0, 1, 3, 0), (2, 0, 3, 1, 1), (14, 0, 1, 1), (5, 0, 1, 3), (4, 0, 2, 1, 1),
    (4, 0, 2, 1, 0), (5, 0, 2, 0), (16, 0, 0, 2, 0), (16, 0, 0, 2, 1), (2, 0, 2, 2, 1),
    (14, 0, 1, 2), (14, 0, 2, 0), (17, 0, 0, 3, 0), (14, 0, 1, 3), (3, 0, 2, 1, 1),
    (2, 0, 2, 2, 0), (16, 0, 0, 1, 1), (3, 0, 2, 1, 0), (17, 0, 0, 3, 1), (15, 0, 0, 0),
    (16, 0, 0, 1, 0), (4, 0, 3, 1, 0), (17, 0, 0, 2, 0), (15, 0, 1, 3), (2, 0, 3, 2, 1),
    (5, 0, 3, 0), (5, 0, 2, 1), (2, 0, 3, 2, 0), (4, 0, 3, 1, 1), (17, 0, 0, 2, 1),
    (3, 0, 3, 1, 1), (14, 0, 3, 0), (16, 0, 1, 3, 0), (16, 0, 1, 3, 1), (4, 0, 2, 2, 0),
    (4, 0, 2, 2, 1), (14, 0, 2, 1), (2, 0, 2, 3, 1), (15, 0, 1, 2), (2, 0, 2, 3, 0),
    (3, 0, 3, 1, 0), (16, 0, 1, 2, 0), (16, 0, 1, 2, 1), (17, 0, 1, 3, 0), (17, 0, 1, 3, 1),
    (3, 0, 2, 2, 0), (15, 0, 1, 1), (3, 0, 2, 2, 1), (17, 0, 0, 1, 0), (17, 0, 0, 1, 1),
    (5, 0, 2, 2), (18, 0, 0), (5, 0, 3, 1), (15, 0, 1, 0), (14, 0, 2, 2), (2, 0, 3, 3, 1),
    (4, 0, 3, 2, 1), (17, 0, 1, 2, 1), (3, 0, 2, 3, 0), (15, 0, 2, 1), (4, 0, 2, 3, 0),
    (2, 0, 3, 3, 0), (4, 0, 2, 3, 1), (17, 0, 1, 2, 0), (16, 0, 1, 1, 0), (3, 0, 2, 3, 1),
    (3, 0, 3, 2, 0), (16, 0, 1, 1, 1), (3, 0, 3, 2, 1), (5, 0, 2, 3), (14, 0, 2, 3), (19, 0, 0),
    (20, 0, 0), (0, 1, 0), (4, 0, 3, 3, 1), (4, 0, 3, 2, 0), (15, 0, 2, 3), (3, 0, 3, 3, 0),
    (16, 0, 2, 3, 0), (17, 0, 1, 1, 0), (17, 0, 1, 1, 1), (16, 0, 2, 3, 1), (18, 0, 1),
    (5, 0, 3, 2), (14, 0, 3, 1), (15, 0, 2, 2), (1, 1, 0), (16, 0, 2, 2, 0), (2, 1, 0, 1, 1),
    (4, 0, 3, 3, 0), (2, 1, 0, 1, 0), (3, 0, 3, 3, 1), (5, 0, 3, 3), (17, 0, 2, 3, 0), (19, 0, 1),
    (16, 0, 2, 2, 1), (20, 0, 1), (14, 0, 3, 2), (0, 1, 1), (14, 0, 3, 3), (3, 1, 0, 1, 0),
    (5, 1, 0, 0), (2, 1, 0, 2, 0), (3, 1, 0, 1, 1), (2, 1, 0, 2, 1), (17, 0, 2, 2, 0),
    (17, 0, 2, 3, 1), (4, 1, 0, 1, 0), (15, 0, 3, 3), (2, 1, 1, 1, 1), (15, 0, 2, 0),
    (14, 1, 0, 0), (16, 0, 3, 3, 1), (1, 1, 1), (16, 0, 3, 3, 0), (4, 1, 0, 2, 1),
    (3, 1, 0, 2, 1), (17, 0, 2, 2, 1), (16, 0, 2, 1, 0), (3, 1, 0, 2, 0), (4, 1, 0, 2, 0),
    (2, 1, 1, 1, 0), (5, 1, 0, 2), (2, 1, 0, 3, 1), (16, 0, 2, 1, 1), (17, 0, 3, 3, 0),
    (15, 0, 3, 2), (2, 1, 0, 3, 0), (17, 0, 3, 3, 1), (4, 1, 0, 1, 1), (16, 0, 3, 2, 1),
    (16, 0, 3, 2, 0), (3, 1, 1, 1, 1), (15, 0, 3, 0), (17, 0, 2, 1, 0), (17, 0, 2, 1, 1),
    (5, 1, 0, 1), (18, 0, 2), (3, 1, 0, 3, 1), (4, 1, 0, 3, 1), (3, 1, 1, 1, 0), (4, 1, 1, 1, 1),
    (15, 0, 3, 1), (14, 1, 0, 1), (4, 1, 1, 1, 0), (3, 1, 0, 3, 0), (5, 1, 1, 0), (14, 1, 1, 0),
    (2, 1, 1, 2, 1), (17, 0, 3, 2, 1), (17, 0, 3, 2, 0), (2, 1, 1, 2, 0), (4, 1, 0, 3, 0),
    (16, 0, 3, 1, 0), (5, 1, 0, 3), (16, 0, 3, 1, 1), (14, 1, 0, 2), (14, 1, 0, 3),
    (3, 1, 1, 2, 1), (3, 1, 1, 2, 0), (19, 0, 2), (20, 0, 2), (0, 1, 2), (15, 1, 0, 3),
    (2, 1, 1, 3, 1), (2, 1, 1, 3, 0), (18, 0, 3), (17, 0, 3, 1, 0), (15, 1, 0, 2), (5, 1, 1, 1),
    (3, 1, 1, 3, 0), (4, 1, 1, 2, 0), (17, 0, 3, 1, 1), (4, 1, 1, 2, 1), (14, 1, 1, 1),
    (16, 1, 0, 3, 0), (16, 1, 0, 3, 1), (1, 1, 2), (2, 1, 2, 1, 0), (3, 1, 1, 3, 1),
    (2, 1, 2, 1, 1), (17, 1, 0, 3, 0), (4, 1, 1, 3, 0), (4, 1, 1, 3, 1), (16, 1, 0, 2, 0),
    (16, 1, 0, 2, 1), (5, 1, 1, 3), (19, 0, 3), (17, 1, 0, 3, 1), (5, 1, 1, 2), (14, 1, 1, 2),
    (20, 0, 3), (0, 1, 3), (14, 1, 1, 3), (3, 1, 2, 1, 0), (4, 1, 2, 1, 0), (4, 1, 2, 1, 1),
    (2, 1, 2, 2, 0), (2, 1, 2, 2, 1), (17, 1, 0, 2, 0), (15, 1, 1, 3), (16, 1, 1, 3, 1),
    (3, 1, 2, 1, 1), (15, 1, 1, 2), (1, 1, 3), (17, 1, 0, 2, 1), (5, 1, 3, 0), (4, 1, 2, 2, 0),
    (3, 1, 2, 2, 0), (5, 1, 2, 1), (16, 1, 1, 3, 0), (15, 1, 0, 1), (4, 1, 2, 2, 1),
    (2, 1, 2, 3, 0), (16, 1, 0, 1, 0), (16, 1, 0, 1, 1), (2, 1, 3, 1, 0), (17, 1, 1, 3, 1),
    (17, 1, 1, 3, 0), (3, 1, 2, 2, 1), (2, 1, 2, 3, 1), (15, 1, 0, 0), (5, 1, 2, 0),
    (2, 1, 3, 1, 1), (14, 1, 2, 0), (14, 1, 2, 1), (17, 1, 0, 1, 1), (17, 1, 0, 1, 0),
    (5, 1, 2, 2), (18, 1, 0), (3, 1, 2, 3, 1), (15, 1, 1, 1), (4, 1, 2, 3, 0), (3, 1, 3, 1, 1),
    (14, 1, 3, 0), (14, 1, 2, 2), (4, 1, 2, 3, 1), (16, 1, 1, 2, 0), (3, 1, 2, 3, 0),
    (16, 1, 1, 2, 1), (3, 1, 3, 1, 0), (17, 1, 1, 2, 0), (5, 1, 2, 3), (17, 1, 1, 2, 1),
    (4, 1, 3, 1, 0), (2, 1, 3, 2, 0), (2, 1, 3, 2, 1), (14, 1, 2, 3), (19, 1, 0), (15, 1, 1, 0),
    (4, 1, 3, 1, 1), (20, 1, 0), (3, 1, 3, 2, 1), (3, 1, 3, 2, 0), (16, 1, 1, 1, 0),
    (15, 1, 2, 3), (16, 1, 2, 3, 0), (5, 1, 3, 1), (16, 1, 1, 1, 1), (17, 1, 1, 1, 0),
    (16, 1, 2, 3, 1), (2, 1, 3, 3, 0), (2, 1, 3, 3, 1), (4, 1, 3, 2, 1), (4, 1, 3, 2, 0), (21, 0),
    (0, 2, 0), (15, 1, 2, 2), (3, 1, 3, 3, 1), (14, 1, 3, 1), (3, 1, 3, 3, 0), (16, 1, 2, 2, 0),
    (5, 1, 3, 2), (14, 1, 3, 2), (4, 1, 3, 3, 1), (18, 1, 1), (17, 1, 1, 1, 1), (17, 1, 2, 3, 0),
    (15, 1, 2, 1), (17, 1, 2, 3, 1), (4, 1, 3, 3, 0), (16, 1, 2, 2, 1), (5, 1, 3, 3),
    (14, 1, 3, 3), (1, 2, 0), (2, 2, 0, 1, 0), (2, 2, 0, 1, 1), (16, 1, 2, 1, 0), (19, 1, 1),
    (20, 1, 1), (17, 1, 2, 2, 1), (15, 1, 3, 3), (16, 1, 3, 3, 0), (17, 1, 2, 2, 0),
    (3, 2, 0, 1, 1), (16, 1, 3, 3, 1), (15, 1, 3, 2), (3, 2, 0, 1, 0), (16, 1, 2, 1, 1), (21, 1),
    (2, 2, 0, 2, 1), (4, 2, 0, 1, 1), (2, 2, 0, 2, 0), (16, 1, 3, 2, 0), (17, 1, 3, 3, 0),
    (15, 1, 2, 0), (4, 2, 0, 1, 0), (2, 2, 0, 3, 1), (0, 2, 1), (17, 1, 3, 3, 1), (3, 2, 0, 2, 0),
    (18, 1, 2), (17, 1, 2, 1, 0), (16, 1, 3, 2, 1), (17, 1, 2, 1, 1), (3, 2, 0, 2, 1),
    (15, 1, 3, 1), (4, 2, 0, 2, 1), (2, 2, 1, 1, 1), (17, 1, 3, 2, 1), (17, 1, 3, 2, 0),
    (16, 1, 3, 1, 0), (15, 1, 3, 0), (2, 2, 1, 1, 0), (16, 1, 3, 1, 1), (5, 2, 0, 0),
    (14, 2, 0, 0), (1, 2, 1), (19, 1, 2), (20, 1, 2), (2, 2, 1, 2, 1), (17, 1, 3, 1, 0),
    (17, 1, 3, 1, 1), (5, 2, 1, 0), (18, 1, 3), (2, 2, 0, 3, 0), (21, 2), (0, 2, 2),
    (2, 2, 1, 2, 0), (3, 2, 1, 1, 1), (3, 2, 1, 1, 0), (19, 1, 3), (20, 1, 3), (4, 2, 1, 1, 0),
    (1, 2, 2), (5, 2, 0, 1), (3, 2, 1, 2, 0), (2, 2, 2, 1, 1), (2, 2, 1, 3, 0), (2, 2, 1, 3, 1),
    (4, 2, 1, 1, 1), (14, 2, 1, 0), (4, 2, 0, 3, 0), (4, 2, 0, 2, 0), (4, 2, 1, 2, 0), (21, 3),
    (0, 2, 3), (14, 2, 0, 1), (4, 2, 0, 3, 1), (5, 2, 2, 0), (2, 2, 2, 1, 0), (3, 2, 1, 2, 1),
    (4, 2, 1, 3, 1), (14, 2, 2, 0), (5, 2, 1, 1), (14, 2, 1, 1), (3, 2, 0, 3, 1), (2, 2, 2, 2, 1),
    (4, 2, 1, 3, 0), (3, 2, 0, 3, 0), (4, 2, 2, 1, 1), (2, 2, 3, 1, 0), (4, 2, 1, 2, 1),
    (2, 2, 2, 3, 1), (2, 2, 3, 1, 1), (3, 2, 1, 3, 1), (1, 2, 3), (4, 2, 2, 1, 0), (5, 2, 0, 2),
    (2, 2, 3, 2, 1), (2, 2, 2, 2, 0), (3, 2, 2, 1, 1), (5, 2, 1, 2), (14, 2, 0, 2),
    (2, 2, 3, 2, 0), (5, 2, 0, 3), (3, 2, 2, 1, 0), (3, 2, 1, 3, 0), (5, 2, 3, 0), (14, 2, 1, 2),
    (4, 2, 3, 1, 0), (14, 2, 0, 3), (3, 2, 3, 1, 1), (5, 2, 2, 1), (14, 2, 2, 1), (5, 2, 1, 3),
    (2, 2, 2, 3, 0), (2, 2, 3, 3, 1), (4, 2, 2, 2, 1), (4, 2, 3, 1, 1), (14, 2, 3, 0),
    (3, 2, 3, 1, 0), (4, 2, 2, 2, 0), (14, 2, 1, 3), (3, 2, 2, 2, 1), (3, 2, 3, 2, 1),
    (4, 2, 3, 2, 0), (4, 2, 2, 3, 1), (4, 2, 3, 2, 1), (2, 2, 3, 3, 0), (3, 2, 2, 2, 0),
    (5, 2, 3, 1), (3, 2, 2, 3, 1), (14, 2, 3, 1), (4, 2, 2, 3, 0), (3, 2, 2, 3, 0),
    (3, 2, 3, 2, 0), (5, 2, 2, 2), (3, 2, 3, 3, 0), (5, 2, 3, 2), (14, 2, 3, 2), (3, 2, 3, 3, 1),
    (5, 2, 2, 3), (4, 2, 3, 3, 1), (4, 2, 3, 3, 0), (14, 2, 2, 2), (14, 2, 2, 3), (5, 2, 3, 3),
    (14, 2, 3, 3),
)
ROUTE = ("S", "H0", "H", "K", "O", "R")
CHAINS = 1 + max(step[2] for step in ORDER if NAMES[step[0]] == "aS")
PLANES = 1 + max(step[3] for step in ORDER if NAMES[step[0]] == "U")
GATHER_SPLIT = ((12, 10, 10, 10), (10, 10, 10, 10), (10, 10, 10, 12))
SCATTER_SPLIT = ((10, 10, 10, 10), (10, 10, 10, 10))


class Plan:
    def __init__(self, experts, groups, rows, width, hidden, slots):
        self.experts, self.groups, self.rows, self.width = experts, groups, rows, width
        self.hidden, self.slots = hidden, slots
        self.capacity = slots // experts
        self.planes = experts // 4
        self.chains = CHAINS
        self.n = rows // self.chains
        self.gather_split = [[self.cut(c) for c in line] for line in GATHER_SPLIT]
        self.scatter_split = [[self.cut(c) for c in line] for line in SCATTER_SPLIT]
        self.lent = max(max(line) for line in self.scatter_split)
        self.rest = width - min(min(line) for line in self.scatter_split)

    def cut(self, sixteenths):
        return self.width * sixteenths // 16

    def fits(self):
        lanes = 128
        whole = (
            self.groups == 2
            and self.experts % 4 == 0
            and 2 * self.experts <= lanes
            and self.planes == PLANES
            and self.rows == lanes
            and self.n % 16 == 0
            and self.width % 2048 == 0
            and self.hidden % (2 * lanes) == 0
            and (2 * self.capacity) % 16 == 0
            and 2 * self.capacity <= 2 * lanes
            and max(self.slots, self.width) <= self.rows * self.experts
            and 2 * self.hidden <= self.width
        )
        return whole and self.bytes() <= 63 * 1024 * 1024

    def bytes(self):
        e, r, d, h, z = self.experts, self.rows, self.width, self.hidden, self.planes
        tokens = 2 * e * r * d * 2 + e * r * d * 2 + e * r * d
        lines = self.chains * self.n * (2 * z * (d + self.rest) + z * self.lent + self.rest) * 2
        return tokens + lines + 2 * d * h * 2 + e * r * h * (4 + 2 + 2) + 3 * r * d * 2 + d * h * 2 + d * h

    def semaphores(self):
        chain = ("rail", "rail2", "over", "sib", "gift", "lend", "sum", "sum2", "last", "swap")
        whole = sum(semaphores_of(self.planes, (kind,)) for kind in chain) * self.chains
        table = sum(semaphores_of(self.planes, (kind,)) for kind in ("rail", "over", "sib"))
        return whole + table + 1


def semaphores_of(planes, kind):
    sizes = {"rail": planes + 1, "rail2": planes + 1, "sum": planes + 1, "sum2": planes + 1}
    sizes.update(over=planes, sib=planes, gift=planes, lend=planes)
    return sizes.get(kind[0], 1)


def fused_kernel(
    plan,
    cot,
    ids,
    gates,
    hidden_hbm,
    up_hbm,
    down_hbm,
    grad_in_hbm,
    grad_w_hbm,
    grad_in,
    grad_w,
    view,
    part,
    gift,
    came,
    came2,
    rung,
    last,
    slope,
    act,
    first,
    third,
    tabs,
    own_tab,
    turn,
    scaled,
    up,
    down,
    total,
    send_sems,
    recv_sems,
    load_sems,
):
    experts, planes, chains, n = plan.experts, plan.planes, plan.chains, plan.n
    width, hidden, cap = plan.width, plan.hidden, plan.capacity
    top = ids.shape[0]
    span = experts * n
    half = width // 2
    me = lax.axis_index("expert")
    token = lax.axis_index("token")
    core = me % 2
    y = (me // 2) % 2
    z = me // 4
    has = {0: z > 0, 1: z < planes - 1}
    up_peer = {"expert": me + 4}
    down_peer = {"expert": me - 4}
    rung_peer = {"expert": me + 2 - 4 * y}
    sib_peer = {"expert": me + 1 - 2 * core}
    far_peer = {"token": 1 - token}
    sources = ((0, up_peer), (1, down_peer))
    full = pl.ds(0, width)

    def sides(split):
        return pl.ds(0, split), pl.ds(split, width - split)


    bases = {}

    def number(key):
        kind, at = key
        if kind not in bases:
            bases[kind] = sum(semaphores_of(planes, name) for name in bases)
        return bases[kind] + at

    def copy(key, src, dst, peer):
        at = number(key)
        return pltpu.make_async_remote_copy(
            src_ref=src,
            dst_ref=dst,
            send_sem=send_sems.at[at],
            recv_sem=recv_sems.at[at],
            device_id=peer,
            device_id_type=MESH,
        )

    def when(cond, action):
        if cond is None:
            action()
        else:
            pl.when(cond)(action)

    pending = {}

    def post(group, cond, key, src, dst, peer):
        when(cond, lambda: copy(key, src, dst, peer).start())
        if group is not None:
            owe(group, cond, key, src)

    def owe(group, cond, key, src):
        pending.setdefault(group, []).append((cond, key, src))

    def drain(group):
        for cond, key, src in pending.pop(group, []):
            when(cond, lambda: copy(key, src, src, sib_peer).wait_send())

    def arrive(cond, key, dst):
        when(cond, lambda: copy(key, dst, dst, sib_peer).wait_recv())

    def both(a, b):
        return b if a is None else (a if b is None else jnp.logical_and(a, b))

    def slot_of(p, yy, cc):
        return 4 * p + 2 * cc + yy

    def origin(way, d):
        return z - d if way == 0 else z + d

    def there(way, d):
        return z >= d if way == 0 else z + d < planes

    mine = slot_of(z, y, core)
    beside = slot_of(z, 1 - y, core)

    def gather(tag, at, src, split):
        group = ("ag", tag)
        whole = split is None
        c1, c2 = sides(width if whole else split)
        rail = lambda way, p: (("rail", tag), p + way)
        rail2 = lambda way, p: (("rail2", tag), p + way)
        across_key = lambda p: (("over", tag), p)
        sib = lambda p: (("sib", tag), p)

        def pair(p, cc):
            return at(slot_of(p, 0, cc), full, 2)

        def start():
            drain(group)
            post(group, None, across_key(z), src, at(mine, full), rung_peer)
            for way, peer in sources:
                post(group, has[1 - way], rail(way, z), src, at(mine, full), peer)
            post(None, None, sib(z), src, at(mine, full), sib_peer)
            owe(group, None, sib(z), pair(z, core))

        def meet():
            block = at(beside, full)
            arrive(None, across_key(z), block)
            if not whole:
                cut = at(beside, c2)
                for way, peer in sources:
                    post(group, has[1 - way], rail2(way, z), cut, cut, peer)
            post(None, None, sib(z), block, block, sib_peer)

        def hop(d, way):
            peer = sources[way][1]
            cond = there(way, d)
            p = origin(way, d)
            block = at(slot_of(p, y, core), full)
            arrive(cond, rail(way, p), block)
            if d + 1 < planes:
                post(group, both(cond, has[1 - way]), rail(way, p), block, block, peer)
            cut = block if whole else at(slot_of(p, y, core), c1)
            post(group, cond, across_key(p), cut, cut, rung_peer)
            post(None, cond, sib(p), block, block, sib_peer)
            owe(group, cond, sib(p), pair(p, core))

        def hop2(d, way):
            peer = sources[way][1]
            cond = there(way, d)
            p = origin(way, d)
            cut = at(slot_of(p, 1 - y, core), c2)
            arrive(cond, rail2(way, p), cut)
            if d + 1 < planes:
                post(group, both(cond, has[1 - way]), rail2(way, p), cut, cut, peer)
            post(None, cond, sib(p), cut, cut, sib_peer)

        def across(d, way):
            cond = there(way, d)
            p = origin(way, d)
            cut = at(slot_of(p, 1 - y, core), full if whole else c1)
            arrive(cond, across_key(p), cut)
            post(None, cond, sib(p), cut, cut, sib_peer)

        def ready(d):
            if d == 0:
                arrive(None, sib(z), pair(z, 1 - core))
                return
            for way in range(2):
                p = origin(way, d)
                arrive(there(way, d), sib(p), pair(p, 1 - core))

        return start, meet, hop, hop2, across, ready

    def plane_at(i):
        low = jnp.minimum(z, planes - 1 - z)
        near = jnp.where(z < planes // 2, 1, -1)
        d = jnp.where(i <= 2 * low, (i + 1) // 2, i - low)
        pair = jnp.where(z % 2 == 0, 1, -1)
        sign = jnp.where(i <= 2 * low, pair * (1 if i % 2 else -1), near)
        return z + sign * d if i else z

    tab_at = lambda slot, cols, count=0: tabs.at[pl.ds(slot, count) if count else slot]

    sources_of = {0: cot, 1: first, 2: third}

    def chain_rows(chain):
        return pl.ds(chain * n, n)

    stages = {}
    for chain in range(chains):
        for f in range(3):

            def at(slot, cols, count=1, f=f, chain=chain):
                rows = pl.ds(pl.multiple_of(chain * span + slot * n, n), count * n)
                return view.at[f % 2, rows, cols]

            src = sources_of[f].at[chain_rows(chain)]
            stages[f, chain] = gather(chain, at, src, plan.gather_split[f][chain])

    def start(f, chain):
        stages[f, chain][0]()
        rows = pl.ds(pl.multiple_of(chain * span + mine * n, n), n)
        view[f % 2, rows, :] = sources_of[f][chain_rows(chain), :]

    hidden_at = view.at[1, pl.ds(0, plan.slots), pl.ds(0, hidden)]
    up_at = view.at[1, pl.ds(0, width), pl.ds(hidden, hidden)]
    loads = [
        pltpu.make_async_copy(hidden_hbm, hidden_at, load_sems.at[0]),
        pltpu.make_async_copy(up_hbm, up_at, load_sems.at[1]),
        pltpu.make_async_copy(down_hbm, down, load_sems.at[2]),
    ]
    turns = 4

    def turn_up(k):
        size = width // turns
        if k == 0:
            loads[1].wait()
        up[:, k * size : (k + 1) * size] = view[
            1, k * size : (k + 1) * size, hidden : 2 * hidden
        ].T
        if k == turns - 1:
            loads[2].wait()

    def make_table():
        lanes = plan.rows
        kind = lax.broadcasted_iota(jnp.int32, (2 * experts, lanes), 0)
        lane = lax.broadcasted_iota(jnp.int32, (lanes, lanes), 1)
        row = lax.broadcasted_iota(jnp.int32, (lanes, lanes), 0)
        match = jnp.zeros(kind.shape, jnp.float32)
        gate = jnp.zeros(kind.shape, jnp.float32)
        for k in range(top):
            name = ids[k : k + 1, :]
            match = match + jnp.where(name == kind, 1.0, 0.0)
            gate = gate + jnp.where(name + experts == kind, gates[k : k + 1, :], 0.0)
        before = jnp.where(row < lane, 1.0, 0.0).astype(jnp.bfloat16)
        rank = jnp.dot(match.astype(jnp.bfloat16), before, preferred_element_type=jnp.float32)
        rank = jnp.where(match > 0.5, rank, -4.0 * lanes)
        table = jnp.where(kind < experts, rank, gate)
        own_tab[...] = table
        tabs[mine] = table

    tile = 256

    def prepare(i):
        p = plane_at(i)
        if i == 0:
            loads[0].wait()
            turn[...] = jnp.zeros_like(turn)
        for j in range(4):
            turn[pl.ds(j, 1), :] = tabs[4 * p + j, pl.ds(me, 1), :]
            turn[pl.ds(4 + j, 1), :] = tabs[4 * p + j, pl.ds(experts + me, 1), :]
        turned = turn[...].T
        spot = lax.broadcasted_iota(jnp.int32, (plan.rows, 2 * cap), 1).astype(jnp.float32)

        @pl.loop(0, hidden // tile)
        def _(step):
            cols = pl.ds(pl.multiple_of(step * tile, tile), tile)
            for yy in range(2):
                rows = pl.ds(pl.multiple_of((4 * p + 2 * yy) * cap, 2 * cap), 2 * cap)
                values = view[1, rows, cols].astype(jnp.float32)
                normal_cdf = 0.5 * (1.0 + lax.erf(values * root_half))
                density = inv_root_two_pi * jnp.exp(-0.5 * values * values)
                steep = normal_cdf + values * density
                active = (values * normal_cdf).astype(jnp.bfloat16)
                high = steep.astype(jnp.bfloat16)
                low = (steep - high.astype(jnp.float32)).astype(jnp.bfloat16)
                for cc in range(2):
                    j = 2 * cc + yy
                    sel = jnp.where(turned[:, j : j + 1] + float(cc * cap) == spot, 1.0, 0.0)
                    sel = sel.astype(jnp.bfloat16)
                    gate = turned[:, 4 + j : 5 + j]
                    pick = lambda rhs: jnp.dot(sel, rhs, preferred_element_type=jnp.float32)
                    steeps = (pick(high) + pick(low)) * gate
                    actives = (pick(active) * gate).astype(jnp.bfloat16)
                    for chain in range(chains):
                        cut = slice(chain * n, (chain + 1) * n)
                        to = pl.multiple_of(chain * span + (4 * p + j) * n, n)
                        slope[pl.ds(to, n), cols] = steeps[cut]
                        act[chain, p, 0, j * n : (j + 1) * n, cols] = actives[cut]

        if i == planes - 1:
            post("act", None, (("act",), 0), act.at[:, :, 0], act.at[:, :, 1], far_peer)

    unit_rows = 8 * n

    def pair_at(i):
        mine_first = z // 2 * 2
        return mine_first if i == 1 else planes - 2 - mine_first

    def apply(f, chain, i):
        if i % 2 == 0:
            return
        base = pl.multiple_of(chain * span + pair_at(i) * 4 * n, unit_rows)
        rows = pl.ds(base, unit_rows)
        if i == 1:
            drain(("rs", chain))
        inner = jnp.dot(view[f % 2, rows, :], down[...], preferred_element_type=jnp.float32)
        scaled[...] = (inner * slope[rows, :]).astype(jnp.bfloat16)
        wide = width // 2

        @pl.loop(0, width // wide)
        def _(step):
            cols = pl.ds(pl.multiple_of(step * wide, wide), wide)
            piece = jnp.dot(scaled[...], up[:, cols], preferred_element_type=jnp.float32)
            part[rows, cols] = piece.astype(jnp.bfloat16)

        for k in (i - 1, i):
            p = plane_at(k)
            away = pl.multiple_of(chain * span + p * 4 * n + (1 - core) * 2 * n, 2 * n)
            post(
                ("rs", chain),
                None,
                (("gift", chain), p),
                part.at[pl.ds(away, 2 * n)],
                gift.at[chain, p],
                sib_peer,
            )

    def part_rows(chain, p, yy):
        return pl.ds(pl.multiple_of(chain * span + slot_of(p, yy, core) * n, n), n)

    patch = 128

    def add_up(cols, terms, store):
        @pl.loop(0, cols.size // patch)
        def _(step):
            offset = pl.multiple_of(step * patch, patch)
            value = None
            for term, shift in terms:
                x = term(pl.ds(pl.multiple_of(offset + shift, patch), patch)).astype(jnp.float32)
                value = x if value is None else value + x
            store(pl.ds(pl.multiple_of(offset + cols.start, patch), patch), value)

    def from_part(chain, p, yy, cols):
        return (lambda at: part[part_rows(chain, p, yy), at]), cols.start

    def to_part(chain, p, yy):
        def store(at, value):
            part[part_rows(chain, p, yy), at] = value.astype(jnp.bfloat16)

        return store

    def from_gift(chain, p, yy, cols):
        rows = pl.ds(pl.multiple_of(yy * n, n), n)
        return (lambda at: gift[chain, p, rows, at]), cols.start

    def from_came(chain, way, p, cols):
        return (lambda at: came[chain, way, p, :, at]), cols.start

    def from_came2(chain, way, p):
        return (lambda at: came2[chain, way, p, :, at]), 0

    def lend(f, chain, i):
        p = plane_at(i)
        c1 = pl.ds(0, plan.scatter_split[f][chain])
        arrive(None, (("gift", chain), p), gift.at[chain, p])
        add_up(
            full,
            [from_part(chain, p, 1 - y, full), from_gift(chain, p, 1 - y, full)],
            to_part(chain, p, 1 - y),
        )
        src = part.at[part_rows(chain, p, 1 - y), c1]
        post(("rs", chain), None, (("lend", chain), p), src, rung.at[chain, p, :, c1], rung_peer)

    def lent(chain, p, c1):
        arrive(None, (("lend", chain), p), rung.at[chain, p, :, c1])

    def carry2(f, chain, d, way):
        c2 = sides(plan.scatter_split[f][chain])[1]
        place = came2.at[chain, way, :, :, pl.ds(0, c2.size)]
        peer = sources[way][1]
        to = z + d if way == 0 else z - d
        cond = there(1 - way, d)
        src = part.at[part_rows(chain, to, 1 - y), c2]

        @pl.when(cond)
        def _():
            if d + 1 < planes:
                arrive(has[way], (("sum2", chain), to + 1 - way), place.at[to])
            add_up(
                c2,
                [from_part(chain, to, 1 - y, c2), from_came2(chain, way, to)],
                to_part(chain, to, 1 - y),
            )
            copy((("sum2", chain), to + 1 - way), src, place.at[to], peer).start()

        owe(("rs", chain), cond, (("sum2", chain), to + 1 - way), src)

    def carry1(f, chain, d, way):
        c1, c2 = sides(plan.scatter_split[f][chain])
        peer = sources[way][1]
        to = z + d if way == 0 else z - d
        cond = there(1 - way, d)
        src = part.at[part_rows(chain, to, y)]

        @pl.when(cond)
        def _():
            lent(chain, to, c1)
            if d + 1 < planes:
                arrive(has[way], (("sum", chain), to + 1 - way), came.at[chain, way, to])
            for cols in (c1, c2):
                terms = [
                    from_part(chain, to, y, cols),
                    from_gift(chain, to, y, cols),
                    from_came(chain, way, to, cols),
                ]
                if cols is c1:
                    terms.append(((lambda at: rung[chain, to, :, at]), 0))
                add_up(cols, terms, to_part(chain, to, y))
            copy((("sum", chain), to + 1 - way), src, came.at[chain, way, to], peer).start()

        owe(("rs", chain), cond, (("sum", chain), to + 1 - way), src)

    def settle2(f, chain):
        c2 = sides(plan.scatter_split[f][chain])[1]
        short = pl.ds(0, c2.size)
        for way in range(2):
            arrive(has[way], (("sum2", chain), z + 1 - way), came2.at[chain, way, z, :, short])
        add_up(
            c2,
            [from_part(chain, z, 1 - y, c2)] + [from_came2(chain, w, z) for w in range(2)],
            to_part(chain, z, 1 - y),
        )
        src = part.at[part_rows(chain, z, 1 - y), c2]
        post(("rs", chain), None, (("last", chain), 0), src, last.at[chain, :, short], rung_peer)

    def finish(f, chain, cols, extra):
        rows = chain_rows(chain)

        def store(at, value):
            term = value.astype(jnp.bfloat16)
            if f == 0:
                first[rows, at] = term
            else:
                whole = (
                    cot[rows, at].astype(jnp.float32)
                    + first[rows, at].astype(jnp.float32)
                    + term.astype(jnp.float32)
                )
                grad_in[rows, at] = whole.astype(jnp.bfloat16)

        terms = [from_part(chain, z, y, cols), from_gift(chain, z, y, cols), extra]
        add_up(cols, terms + [from_came(chain, w, z, cols) for w in range(2)], store)

    def settle1(f, chain):
        c1 = pl.ds(0, plan.scatter_split[f][chain])
        lent(chain, z, c1)
        for way in range(2):
            arrive(has[way], (("sum", chain), z + 1 - way), came.at[chain, way, z])
        finish(f, chain, c1, ((lambda at: rung[chain, z, :, at]), 0))

    def settle(f, chain):
        c2 = sides(plan.scatter_split[f][chain])[1]
        arrive(None, (("last", chain), 0), last.at[chain, :, pl.ds(0, c2.size)])
        finish(f, chain, c2, ((lambda at: last[chain, :, at]), 0))
        if f == 1:
            swap(chain)
            rows = chain_rows(chain)
            save(chain, grad_in.at[rows], grad_in_hbm.at[rows])

    saved = []

    def save(at, src, dst):
        copy_out = pltpu.make_async_copy(src, dst, load_sems.at[at])
        copy_out.start()
        saved.append(copy_out)

    def swap(chain):
        rows = chain_rows(chain)
        away = pl.ds(pl.multiple_of((1 - token) * half, half), half)
        keep = pl.ds(pl.multiple_of(token * half, half), half)
        post(
            "swap",
            None,
            (("swap", chain), 0),
            grad_in.at[rows, away],
            third.at[rows, pl.ds(half, half)],
            far_peer,
        )
        third[rows, pl.ds(0, half)] = grad_in[rows, keep]

    def swapped(chain):
        arrive(None, (("swap", chain), 0), third.at[chain_rows(chain), pl.ds(half, half)])

    def weigh(chain, i, end):
        if i % 2 == 0:
            return
        p = pair_at(i)
        start = pl.multiple_of(chain * span + p * 4 * n, unit_rows)
        upper = pl.ds(start, 4 * n)
        lower = pl.ds(pl.multiple_of(start + 4 * n, 4 * n), 4 * n)

        @pl.loop(0, half // tile)
        def _(step):
            base = pl.multiple_of(step * tile, tile)
            out = pl.ds(base, tile)
            left = pl.ds(base, tile)
            right = pl.ds(pl.multiple_of(half + base, tile), tile)
            value = lax.dot_general(
                jnp.concatenate(
                    [view[0, rows, cols] for rows in (upper, lower) for cols in (left, right)],
                    axis=0,
                ),
                act[chain, pl.ds(p, 2)].reshape(2 * unit_rows, hidden),
                (((0,), (0,)), ((), ())),
                preferred_element_type=jnp.float32,
            )
            if end:
                grad_w[out, :] = ((total[out, :] + value) * grad_scale).astype(jnp.bfloat16)
                pltpu.make_async_copy(
                    grad_w.at[out], grad_w_hbm.at[out], load_sems.at[chains + step]
                ).start()
            else:
                total[out, :] += value

        if end:
            for step in range(half // tile):
                out = pl.ds(step * tile, tile)
                saved.append(
                    pltpu.make_async_copy(
                        grad_w.at[out], grad_w_hbm.at[out], load_sems.at[chains + step]
                    )
                )

    for load in loads:
        load.start()
    barrier = pltpu.get_barrier_semaphore()
    for cond, peer in (
        (has[1], up_peer),
        (has[0], down_peer),
        (None, rung_peer),
        (None, sib_peer),
        (None, far_peer),
    ):
        when(
            cond,
            lambda: pl.semaphore_signal(barrier, inc=1, device_id=peer, device_id_type=MESH),
        )
    make_table()
    count = 3 + jnp.where(z > 0, 1, 0) + jnp.where(z < planes - 1, 1, 0)
    pl.semaphore_wait(barrier, count)

    def clear():
        total[...] = jnp.zeros_like(total)
        for way in range(2):

            @pl.when(jnp.logical_not(has[way]))
            def _():
                for chain in range(chains):
                    came[chain, way] = jnp.zeros(came.shape[2:], came.dtype)
                    came2[chain, way] = jnp.zeros(came2.shape[2:], came2.dtype)

    units = [0]

    def unit(f, chain, i):
        if f < 2:
            apply(f, chain, i)
            return
        if units[0] == 0:
            arrive(None, (("act",), 0), act.at[:, :, 1])
        units[0] += 1
        weigh(chain, i, units[0] == chains * planes)

    tab = gather("tab", tab_at, own_tab, None)
    routes = {("a", f, c): stages[f, c] for f in range(3) for c in range(chains)}
    routes["t", 0, 0] = tab
    actions = {
        "P": prepare,
        "X": turn_up,
        "N": clear,
        "U": unit,
        "L": lend,
        "D": carry2,
        "C": carry1,
        "T2": settle2,
        "T1": settle1,
        "T": settle,
        "W": swapped,
        "aS": start,
        "tS": lambda f, c: tab[0](),
    }
    for kind, *args in ORDER:
        name = NAMES[kind]
        with jax.named_scope("_".join([name] + [str(a) for a in args])):
            if name in actions:
                actions[name](*args)
            else:
                routes[(name[0],) + tuple(args[:2])][ROUTE.index(name[1:])](*args[2:])
    for group in list(pending):
        drain(group)
    for copy_out in saved:
        copy_out.wait()


def fused(plan, cotangent, expert_ids, gate_values, hidden_pre, up_weight, down_weight):
    experts, planes, chains, n = plan.experts, plan.planes, plan.chains, plan.n
    width, hidden, rows = plan.width, plan.hidden, plan.rows
    half = width // 2
    low, dma = jnp.bfloat16, pltpu.SemaphoreType.DMA
    vmem = pl.BlockSpec(memory_space=pltpu.VMEM)
    hbm = pl.BlockSpec(memory_space=pl.ANY)
    count = plan.semaphores()
    return pl.pallas_call(
        functools.partial(fused_kernel, plan),
        out_shape=[
            jax.ShapeDtypeStruct((rows, width), low),
            jax.ShapeDtypeStruct((half, hidden), low),
        ],
        in_specs=[vmem, vmem, vmem, hbm, hbm, hbm],
        out_specs=[hbm, hbm],
        scratch_shapes=[
            pltpu.VMEM((rows, width), low),
            pltpu.VMEM((half, hidden), low),
            pltpu.VMEM((2, chains * experts * n, width), low),
            pltpu.VMEM((chains * experts * n, width), low),
            pltpu.VMEM((chains, planes, 2 * n, width), low),
            pltpu.VMEM((chains, 2, planes, n, width), low),
            pltpu.VMEM((chains, 2, planes, n, plan.rest), low),
            pltpu.VMEM((chains, planes, n, plan.lent), low),
            pltpu.VMEM((chains, n, plan.rest), low),
            pltpu.VMEM((chains * experts * n, hidden), jnp.float32),
            pltpu.VMEM((chains, planes, 2, 4 * n, hidden), low),
            pltpu.VMEM((rows, width), low),
            pltpu.VMEM((rows, width), low),
            pltpu.VMEM((experts, 2 * experts, rows), jnp.float32),
            pltpu.VMEM((2 * experts, rows), jnp.float32),
            pltpu.VMEM((rows, rows), jnp.float32),
            pltpu.VMEM((8 * n, hidden), low),
            pltpu.VMEM((hidden, width), low),
            pltpu.VMEM((width, hidden), low),
            pltpu.VMEM((half, hidden), jnp.float32),
            dma((count,)),
            dma((count,)),
            dma((max(3, chains + half // 256),)),
        ],
        compiler_params=pltpu.CompilerParams(
            collective_id=5, has_side_effects=True, vmem_limit_bytes=67_043_328
        ),
        cost_estimate=pl.CostEstimate(
            flops=40_000_000_000, bytes_accessed=20_000_000, transcendentals=0
        ),
        name="fused",
    )(cotangent, expert_ids.T, gate_values.T, hidden_pre, up_weight, down_weight)


def hand_on_kernel(count, pieces, *refs):
    sources, targets, held = refs[:count], refs[count : 2 * count], refs[2 * count : 3 * count]
    into, out = refs[3 * count :]
    loads, stores = [], []
    for i in range(count):
        size = sources[i].shape[0] // pieces
        for k in range(pieces):
            rows = pl.ds(k * size, size)
            at = i * pieces + k
            loads.append(
                pltpu.make_async_copy(sources[i].at[rows], held[i].at[rows], into.at[at])
            )
            stores.append(
                pltpu.make_async_copy(held[i].at[rows], targets[i].at[rows], out.at[at])
            )
    for load in loads:
        load.start()
    for load, store in zip(loads, stores):
        load.wait()
        store.start()
    for store in stores:
        store.wait()


def hand_on(arrays):
    count, pieces = len(arrays), 4
    place = pl.BlockSpec(memory_space=pl.ANY)
    dma = pltpu.SemaphoreType.DMA
    return pl.pallas_call(
        functools.partial(hand_on_kernel, count, pieces),
        out_shape=[jax.ShapeDtypeStruct(a.shape, a.dtype) for a in arrays],
        in_specs=[place] * count,
        out_specs=[place] * count,
        scratch_shapes=[pltpu.VMEM(a.shape, a.dtype) for a in arrays]
        + [dma((count * pieces,)), dma((count * pieces,))],
        name="hand_on",
    )(*arrays)


def body(cotangent, expert_ids, gate_values, hidden_pre, up_weight, down_weight):
    plan = Plan(
        lax.axis_size("expert"),
        lax.axis_size("token"),
        cotangent.shape[0],
        cotangent.shape[1],
        hidden_pre.shape[2],
        hidden_pre.shape[1],
    )
    if not plan.fits():
        return staged(cotangent, expert_ids, gate_values, hidden_pre, up_weight, down_weight)
    input_grad, grad_out = fused(
        plan, cotangent, expert_ids, gate_values, hidden_pre[0], up_weight[0], down_weight[0]
    )
    input_grad, grad_out = hand_on([input_grad, grad_out])
    return (input_grad, grad_out[None])


def solution(mesh):
    in_specs = (
        P(("expert", "token"), None),
        P(("expert", "token"), None),
        P(("expert", "token"), None),
        P("expert", "token", None),
        P("expert", None, None),
        P("expert", None, None),
    )
    out_specs = (P(("expert", "token"), None), P("expert", "token", None))
    return jax.shard_map(body, mesh=mesh, in_specs=in_specs, out_specs=out_specs, check_vma=False)
```
